256 devices in a mesh: item: 128 (over x, y_hi, z, core), grp: 2 (over y_lo).
Axes of the slice: x: 4, y: 4 (y_hi: 2, y_lo: 2; y = y_hi * 2 + y_lo), z: 8, core: 2. Of those that a mesh axis runs over, the one named last changes fastest.
Arguments:
- hidden: bfloat16 [768, 256], P(('grp', 'item')), may hold values from -400 to 400
- item_table: bfloat16 [1048576, 256], P('item'), may hold values from -1.5 to 1.5
- targets: int32 [768], P(('grp', 'item')), may hold values from 0 to 1048575
- lengths: int32 [2, 16], replicated, may hold values from 1 to 96, 384 in all within a row
Outputs:
- row_loss: float32 [768], P(('grp', 'item'))
- hidden_grad: bfloat16 [768, 256], P(('grp', 'item'))
- table_grad: bfloat16 [1048576, 256], P(('item', 'grp'))
The draws below stay inside these ranges and needn't reach their ends.
Inputs may be any that keep to these rules, and one draw needn't show every extreme that they name: Each row holds the lengths of the 16 user sequences that fill one group's 384 positions in order, and sums to 384.
All inputs are finite; a program needn't handle non-finite values.
Results may differ from the reference program's by a relative error of at most 0.0047.
Values may be sent and summed in bfloat16 or wider, within the bound.
No kernel may reach another device: no remote copies, remote signals or barrier semaphores. Data moves between devices by JAX's collectives and lax.ppermute only.
A program may use at most 64 MiB of HBM per device.

```python
import math
import jax
import jax.numpy as jnp
import numpy as np
from jax import lax

D = 256
ITEM_DEV = 8192
TOKG = 384
SEQG = 16
TOKENS = 768
ITEMS = 1048576
MAXLEN = 96
N_GRP = 2


def draw_common(key):
    table_key = jax.random.fold_in(jax.random.fold_in(key, 7), 0)
    state_key = jax.random.fold_in(jax.random.fold_in(key, 7), 1)
    item_key = jax.random.fold_in(jax.random.fold_in(key, 7), 3)
    noise_key = jax.random.fold_in(jax.random.fold_in(key, 7), 4)
    place_key = jax.random.fold_in(jax.random.fold_in(key, 7), 5)
    table = 0.2 * jax.random.truncated_normal(table_key, -5.0, 5.0, (ITEMS, D), jnp.float32)
    states = jax.random.truncated_normal(state_key, -6.0, 6.0, (TOKENS, D), jnp.float32)
    chosen = jax.random.randint(item_key, (8,), 0, ITEMS // 2)
    partner = chosen + ITEMS // 2
    strength = jnp.array([120.0, 220.0, 300.0, 160.0, 260.0, 120.0, 220.0, 300.0], jnp.float32)
    anchor = table[chosen]
    anchor_sq = jnp.sum(anchor * anchor, axis=1, keepdims=True)
    noise = jax.random.normal(noise_key, (8, D), jnp.float32)
    noise = noise - jnp.sum(noise * anchor, axis=1, keepdims=True) / anchor_sq * anchor
    partner_rows = anchor * (1.0 + 2.0 / strength[:, None]) + 0.05 * jnp.clip(noise, -5.0, 5.0)
    table = table.at[partner].set(partner_rows)
    offsets = jax.random.randint(place_key, (8,), 0, TOKENS // 8)
    rows_hit = TOKENS // 8 * jnp.arange(8) + offsets
    states = states.at[rows_hit].set(strength[:, None] * anchor / anchor_sq)
    return (table, states)


def draw_hidden(key, part):
    return draw_common(key)[1].astype(jnp.bfloat16)


def draw_item_table(key, part):
    return draw_common(key)[0].astype(jnp.bfloat16)


def set_ends(values, stream_key, smallest, top_value):
    longest = values.shape.index(max(values.shape))
    spots = []
    for shift in (0, 1):
        where = [jax.random.randint(jax.random.fold_in(stream_key, axis), (), 0, length) for axis, length in enumerate(values.shape)]
        where[longest] = (where[longest] + shift) % values.shape[longest]
        spots.append(tuple(where))
    return values.at[spots[0]].set(smallest).at[spots[1]].set(top_value)


def wide_ids(rng, dims, number_of, lean):
    loads = [min(1 << octave, number_of + 1 - (1 << octave)) * (1 << 20) // math.isqrt((1 << octave) ** lean) + 1 for octave in range((number_of + 1).bit_length()) if 1 << octave <= number_of]
    scale = 1 + sum(loads) // (1 << 30)
    listing = np.cumsum(np.array([max(1, weight // scale) for weight in loads]))
    lot = jax.random.randint(jax.random.fold_in(rng, 1), dims, 0, int(listing[len(loads) - 1]))
    start = jnp.left_shift(1, jnp.searchsorted(jnp.asarray(listing, jnp.int32), lot, side="right").astype(jnp.int32))
    rank = start - 1 + jax.random.randint(jax.random.fold_in(rng, 4), dims, 0, 1 << 30) % jnp.minimum(start, number_of + 1 - start)
    return jax.random.permutation(jax.random.fold_in(rng, 2), number_of)[rank].astype(jnp.int32)


def split_up(count, total, most, skew):
    weights = [(1 << 20) // math.isqrt(grade ** skew) + 1 for grade in range(2, count + 1)]
    rest, given = total - most - (count - 1), [1] * (count - 1)
    while rest > 0:
        candidates = [i for i in range(count - 1) if given[i] < most]
        mass, left = sum([weights[i] for i in candidates]), rest
        for i in candidates:
            more = min(most - given[i], max(1, left * weights[i] // mass), rest)
            given[i] = given[i] + more
            rest = rest - more
    return np.array([most] + given)


def uneven(key, count, total, bound, slope):
    if count == 2:
        one = jax.random.randint(key, (), max(1, total - bound), min(bound, total - 1) + 1)
        return jnp.stack([one, total - one])
    tallies = jnp.asarray(split_up(count, total, bound, slope), jnp.int32)
    pairs = (count - 1) // 2
    source_of, taker = tallies[1:1 + 2 * pairs:2], tallies[2:2 + 2 * pairs:2]
    margin = jnp.minimum(source_of - 1, bound - taker)
    shifted = jax.random.randint(jax.random.fold_in(key, 1), (pairs,), 0, 1 << 20) % (margin + 1)
    tallies = tallies.at[1:1 + 2 * pairs:2].set(source_of - shifted).at[2:2 + 2 * pairs:2].set(taker + shifted)
    return tallies[jax.random.permutation(jax.random.fold_in(key, 2), count)]


def setup_inputs(seed: int = 0) -> dict:
    streams_of = jax.random.split(jax.random.key(seed), 5)
    return {
        "hidden": draw_hidden(jax.random.fold_in(streams_of[4], 71), 0),
        "item_table": draw_item_table(jax.random.fold_in(streams_of[4], 71), 0),
        "targets": set_ends(wide_ids(streams_of[2], (TOKENS,), ITEMS, 2), jax.random.fold_in(streams_of[2], 3), 0, ITEMS - 1).astype(jnp.int32),
        "lengths": jax.vmap(lambda own: uneven(own, SEQG, TOKG, MAXLEN, 2))(jax.random.split(streams_of[3], N_GRP)).reshape((N_GRP, SEQG)).astype(jnp.int32),
    }


def row_weights(lengths, group_rows):
    seq_count = lengths.shape[1]
    seq_ends = jnp.cumsum(lengths, axis=1)
    starts = seq_ends - lengths
    places = jnp.arange(group_rows, dtype=jnp.int32)
    inside = (places[None, :, None] >= starts[:, None, :]) & (places[None, :, None] < seq_ends[:, None, :])
    row_length = jnp.sum(jnp.where(inside, lengths[:, None, :].astype(jnp.float32), jnp.float32(0.0)), axis=2)
    return ((group_rows / seq_count) / row_length).reshape(-1)


def reference(hidden, item_table, targets, lengths):
    token_count = hidden.shape[0]
    group_rows = token_count // lengths.shape[0]
    states = hidden.astype(jnp.float32)
    block_count = ITEMS // ITEM_DEV
    blocks = item_table.reshape(block_count, ITEM_DEV, D)
    block_starts = ITEM_DEV * jnp.arange(block_count, dtype=jnp.int32)

    def visit(carried, block_pair):
        highest, running, picked = carried
        item_block, block_start = block_pair
        scores = jnp.dot(states, item_block.astype(jnp.float32).T, precision=lax.Precision.HIGHEST)
        new_max = jnp.maximum(highest, jnp.max(scores, axis=1))
        running = running * jnp.exp(highest - new_max) + jnp.sum(jnp.exp(scores - new_max[:, None]), axis=1)
        columns = block_start + jnp.arange(ITEM_DEV, dtype=jnp.int32)
        matched = targets[:, None] == columns[None, :]
        picked = picked + jnp.sum(jnp.where(matched, scores, jnp.float32(0.0)), axis=1)
        return (new_max, running, picked), None

    start_stats = (jnp.full((token_count,), -jnp.inf, dtype=jnp.float32),
                   jnp.zeros((token_count,), jnp.float32), jnp.zeros((token_count,), jnp.float32))
    final_stats, unused = lax.scan(visit, start_stats, (blocks, block_starts))
    row_max, exp_total, target_score = final_stats
    log_total = row_max + jnp.log(exp_total)
    row_loss = log_total - target_score
    weight = row_weights(lengths, group_rows)

    def back_visit(state_grad, block_pair):
        item_block, block_start = block_pair
        block_f = item_block.astype(jnp.float32)
        scores = jnp.dot(states, block_f.T, precision=lax.Precision.HIGHEST)
        columns = block_start + jnp.arange(ITEM_DEV, dtype=jnp.int32)
        matched = (targets[:, None] == columns[None, :]).astype(jnp.float32)
        signal = (weight[:, None] * (jnp.exp(scores - log_total[:, None]) - matched)).astype(jnp.bfloat16)
        signal_f = signal.astype(jnp.float32)
        state_grad = state_grad + jnp.dot(signal_f, block_f, precision=lax.Precision.HIGHEST)
        item_grad = jnp.dot(signal_f.T, states, precision=lax.Precision.HIGHEST)
        return state_grad, item_grad.astype(jnp.bfloat16)

    state_grad, item_grads = lax.scan(back_visit, jnp.zeros((token_count, D), jnp.float32), (blocks, block_starts))
    return row_loss, state_grad.astype(jnp.bfloat16), item_grads.reshape(ITEMS, D)
```

```python
import jax
import jax.numpy as jnp
from jax import lax
from jax.experimental import pallas as pl
from jax.experimental.pallas import tpu as pltpu
from jax.sharding import Mesh
from jax.sharding import PartitionSpec as P

ITEM = ("x", "yh", "z", "core")
GRP_ITEM = ("grp", "x", "yh", "z", "core")
ITEM_GRP = ("x", "yh", "z", "core", "grp")
PLANE = ("x", "yh", "grp")
CHIPS = ("x", "yh", "grp", "z")
DIGIT = 128
BLOCK = 512
F32 = jnp.float32
BF16 = jnp.bfloat16


def sent_to_all(x, axes):
    length = lax.axis_size(axes)
    return lax.all_to_all(jnp.broadcast_to(x[None], (length, *x.shape)), axes, 0, 0, tiled=True)


def from_pair(x):
    return lax.ppermute(x, "core", [(0, 1), (1, 0)])


def gathered(hidden, targets):
    rows, width = hidden.shape
    digits = jnp.stack([targets % DIGIT, targets // DIGIT % DIGIT, targets // DIGIT**2])
    digits = jnp.pad(digits.reshape(-1), (0, width - 3 * rows)).astype(BF16)
    mine = sent_to_all(jnp.concatenate([hidden, digits[None]]), CHIPS)
    other = from_pair(mine)
    first = lax.axis_index("core") == 0
    both = jnp.concatenate([jnp.where(first, mine, other), jnp.where(first, other, mine)])
    states = both[:, :rows].reshape(-1, width)
    digits = both[:, rows, : 3 * rows].reshape(-1, 3, rows).astype(jnp.int32)
    target_ids = digits[:, 0] + DIGIT * digits[:, 1] + DIGIT**2 * digits[:, 2]
    return states, target_ids.reshape(1, -1)


def weights_for(lengths, rows):
    groups, seq_count = lengths.shape
    sizes = [lax.axis_size(axis) for axis in ("core", "x", "yh", "grp", "z")]
    core, x, yh, grp, z, k = jnp.unravel_index(
        jnp.arange(sizes[0] * sizes[1] * sizes[2] * sizes[3] * sizes[4] * rows), (*sizes, rows)
    )
    place = (((x * sizes[2] + yh) * sizes[4] + z) * sizes[0] + core) * rows + k
    group_rows = place.shape[0] // groups
    before = jnp.arange(seq_count)[:, None] < jnp.arange(seq_count)[None, :]
    starts = jnp.sum(jnp.where(before[None], lengths[:, :, None], 0), axis=1)
    inside = (
        (grp[:, None, None] == jnp.arange(groups)[None, :, None])
        & (place[:, None, None] >= starts[None])
        & (place[:, None, None] < (starts + lengths)[None])
    )
    row_length = jnp.sum(jnp.where(inside, lengths[None].astype(F32), F32(0.0)), axis=(1, 2))
    return (group_rows / seq_count / row_length).reshape(1, -1)


def share_kernel(half_ref, target_ref, states_ref, items_ref, grad_ref, rows_ref, log_ref, high, total, grad, picked):
    step = pl.program_id(0)
    block = items_ref.shape[0]

    @pl.when(step == 0)
    def _():
        high[...] = jnp.full(high.shape, -jnp.inf, F32)
        total[...] = jnp.zeros(total.shape, F32)
        grad[...] = jnp.zeros(grad.shape, F32)
        picked[...] = jnp.zeros(picked.shape, F32)

    items = items_ref[...]
    scores = lax.dot_general(
        items, states_ref[...], (((1,), (1,)), ((), ())), preferred_element_type=F32
    )
    top = jnp.maximum(high[...], jnp.max(scores, axis=0, keepdims=True))
    shrink = jnp.exp(high[...] - top)
    parts = jnp.exp(scores - top)
    total[...] = total[...] * shrink + jnp.sum(parts, axis=0, keepdims=True)
    high[...] = top
    place = lax.broadcasted_iota(jnp.int32, parts.shape, 0)
    matched = place == target_ref[...] - step * block
    others = jnp.where(matched, 0.0, parts).astype(BF16)
    hot = jnp.where(matched, 1.0, 0.0).astype(BF16)
    across = items.T
    grad[...] = grad[...] * shrink + jnp.dot(across, others, preferred_element_type=F32)
    picked[...] += jnp.dot(across, hot, preferred_element_type=F32)

    @pl.when(step == pl.num_programs(0) - 1)
    def _():
        log_sum = high[...] + jnp.log(total[...])
        log_ref[...] = log_sum
        grad_ref[...] = grad[...] * jnp.exp(high[...] - log_sum)
        rows_ref[...] = picked[...].astype(BF16)


def shares(half, target_place, states, item_table):
    own = item_table.shape[0] // 2
    block = min(BLOCK, own)
    width, count = states.shape[1], states.shape[0]
    steps = own // block
    whole = lambda i, half: (0, 0)
    return pl.pallas_call(
        share_kernel,
        name="shares",
        out_shape=(
            jax.ShapeDtypeStruct((width, count), F32),
            jax.ShapeDtypeStruct((width, count), BF16),
            jax.ShapeDtypeStruct((1, count), F32),
        ),
        grid_spec=pltpu.PrefetchScalarGridSpec(
            num_scalar_prefetch=1,
            grid=(steps,),
            in_specs=[
                pl.BlockSpec((1, count), whole),
                pl.BlockSpec((count, width), whole),
                pl.BlockSpec((block, width), lambda i, half: (half[0] * steps + i, 0)),
            ],
            out_specs=[
                pl.BlockSpec((width, count), whole),
                pl.BlockSpec((width, count), whole),
                pl.BlockSpec((1, count), whole),
            ],
            scratch_shapes=[
                pltpu.VMEM((1, count), F32),
                pltpu.VMEM((1, count), F32),
                pltpu.VMEM((width, count), F32),
                pltpu.VMEM((width, count), F32),
            ],
        ),
        compiler_params=pltpu.CompilerParams(dimension_semantics=("arbitrary",)),
    )(half, target_place, states, item_table)


def table_kernel(half_ref, target_ref, log_ref, weight_ref, states_ref, items_ref, out_ref):
    step = pl.program_id(0)
    block = items_ref.shape[0]
    states = states_ref[...]
    scores = lax.dot_general(
        items_ref[...], states, (((1,), (1,)), ((), ())), preferred_element_type=F32
    )
    parts = jnp.exp(scores - log_ref[...])
    place = lax.broadcasted_iota(jnp.int32, parts.shape, 0)
    matched = place == target_ref[...] - step * block
    signal = (weight_ref[...] * jnp.where(matched, parts - 1.0, parts)).astype(BF16)
    out_ref[...] = jnp.dot(signal, states, preferred_element_type=F32).astype(BF16)


def table_gradient(half, target_place, log_total, weight, states, item_table):
    own = item_table.shape[0] // 2
    block = min(BLOCK, own)
    width, count = states.shape[1], states.shape[0]
    steps = own // block
    whole = lambda i, half: (0, 0)
    line = pl.BlockSpec((1, count), whole)
    return pl.pallas_call(
        table_kernel,
        name="table_gradient",
        out_shape=jax.ShapeDtypeStruct((own, width), BF16),
        grid_spec=pltpu.PrefetchScalarGridSpec(
            num_scalar_prefetch=1,
            grid=(steps,),
            in_specs=[
                line,
                line,
                line,
                pl.BlockSpec((count, width), whole),
                pl.BlockSpec((block, width), lambda i, half: (half[0] * steps + i, 0)),
            ],
            out_specs=pl.BlockSpec((block, width), lambda i, half: (i, 0)),
        ),
        compiler_params=pltpu.CompilerParams(dimension_semantics=("arbitrary",)),
    )(half, target_place, log_total, weight, states, item_table)


def thirds(x):
    high = lax.reduce_precision(x, 8, 7)
    rest = x - high
    middle = lax.reduce_precision(rest, 8, 7)
    return jnp.concatenate([high, middle, rest - middle]).astype(BF16)


def merged_logs(parts):
    top = jnp.max(parts, axis=0)
    return top + jnp.log(jnp.sum(jnp.exp(parts - top[None]), axis=0))


def exchanged(grad, picked, logs, axes):
    length = lax.axis_size(axes)
    width = grad.shape[-1]
    lines = thirds(logs).reshape(-1, width)
    lines = jnp.broadcast_to(lines[None], (length, *lines.shape))
    sent = jnp.concatenate(
        [grad.reshape(length, -1, width).astype(BF16), picked.reshape(length, -1, width), lines],
        axis=1,
    )
    arrived = lax.all_to_all(sent, axes, 0, 0, tiled=True)
    rows = grad.shape[0] // length
    given = arrived[:, 2 * rows :].astype(F32).reshape(length, 3, -1).sum(axis=1)
    return arrived[:, :rows].astype(F32), arrived[:, rows : 2 * rows], given


def local(hidden, item_table, targets, lengths):
    rows = hidden.shape[0]
    items_local = item_table.shape[0]
    core = lax.axis_index("core")
    group = lax.axis_index("grp")
    half = group.reshape(1).astype(jnp.int32)
    states, target_ids = gathered(hidden, targets)
    weight = weights_for(lengths, rows)
    first_own = lax.axis_index(ITEM) * items_local + group * (items_local // 2)
    target_place = target_ids - first_own
    count = states.shape[0]
    grad, picked, logs = shares(half, target_place, states, item_table)
    part = count // 2
    own_at = core * part
    other_at = part - own_at
    take = lambda x, at: lax.dynamic_slice_in_dim(x, at, part, 1)
    other_logs = from_pair(logs)
    other_grad = from_pair(take(grad, other_at))
    other_picked = from_pair(take(picked, other_at))
    both_logs = merged_logs(jnp.stack([logs, other_logs]))
    scale = lambda x: jnp.exp(take(x, own_at) - take(both_logs, own_at))
    grad = (take(grad, own_at) * scale(logs) + other_grad * scale(other_logs)).T
    picked = (take(picked, own_at) + other_picked).T
    at = own_at
    logs = both_logs.reshape(-1)
    for axes in (PLANE, "z"):
        grads, pickeds, given = exchanged(grad, picked, logs, axes)
        logs = merged_logs(given)
        kept = grads.shape[1]
        at = at + lax.axis_index(axes) * kept
        scale = jnp.exp(
            lax.dynamic_slice_in_dim(given, at, kept, 1) - lax.dynamic_slice_in_dim(logs, at, kept)
        )
        grad = jnp.sum(grads * scale[:, :, None], axis=0)
        picked = jnp.sum(pickeds.astype(F32), axis=0).astype(BF16)
    own_logs = lax.dynamic_slice_in_dim(logs, at, rows)
    own_weight = lax.dynamic_slice_in_dim(weight[0], at, rows)
    picked = picked.astype(F32)
    target_score = jnp.sum(hidden.astype(F32) * picked, axis=1)
    row_loss = own_logs - target_score
    pull = lax.reduce_precision(own_weight * (jnp.exp(target_score - own_logs) - 1.0), 8, 7)
    hidden_grad = (own_weight[:, None] * grad + pull[:, None] * picked).astype(BF16)
    table_grad = table_gradient(half, target_place, logs[None], weight, states, item_table)
    return (row_loss, hidden_grad, table_grad)


def mapped(split):
    return jax.shard_map(
        local,
        mesh=split,
        in_specs=(P(GRP_ITEM, None), P(ITEM, None), P(GRP_ITEM), P()),
        out_specs=(P(GRP_ITEM), P(GRP_ITEM, None), P(ITEM_GRP, None)),
        check_vma=False,
    )


def solution(mesh):
    return mapped(
        Mesh(
            mesh.devices.reshape(4, 2, 8, 2, mesh.shape["grp"]),
            ("x", "yh", "z", "core", "grp"),
        )
    )
```

```python
import functools

import jax
import jax.numpy as jnp
from jax import lax
from jax.experimental import pallas as pl
from jax.experimental.pallas import tpu as pltpu
from jax.sharding import Mesh
from jax.sharding import PartitionSpec as P

ITEM = ("x", "yh", "z", "core")
GRP_ITEM = ("grp", "x", "yh", "z", "core")
ITEM_GRP = ("x", "yh", "z", "core", "grp")
PLANE = ("x", "yh", "grp")
CHIPS = ("x", "yh", "grp", "z")
DIGIT = 128
BLOCK = 512
VMEM_LIMIT = 40 << 20
F32 = jnp.float32
BF16 = jnp.bfloat16


def sent_to_all(x, axes):
    length = lax.axis_size(axes)
    return lax.all_to_all(jnp.broadcast_to(x[None], (length, *x.shape)), axes, 0, 0, tiled=True)


def from_pair(x):
    return lax.ppermute(x, "core", [(0, 1), (1, 0)])


def gathered(hidden, targets):
    rows, width = hidden.shape
    digits = jnp.stack([targets % DIGIT, targets // DIGIT % DIGIT, targets // DIGIT**2])
    digits = jnp.pad(digits.reshape(-1), (0, width - 3 * rows)).astype(BF16)
    mine = sent_to_all(jnp.concatenate([hidden, digits[None]]), CHIPS)
    mine = jnp.swapaxes(mine, 0, 1)
    return mine, from_pair(mine)


def weights_for(lengths, rows):
    groups, seq_count = lengths.shape
    cores, x, yh, grps, z = (lax.axis_size(axis) for axis in ("core", "x", "yh", "grp", "z"))
    half, k, at_x, at_yh, at_grp, at_z = jnp.unravel_index(
        jnp.arange(cores * rows * x * yh * grps * z), (cores, rows, x, yh, grps, z)
    )
    core = (half + lax.axis_index("core")) % cores
    place = (((at_x * yh + at_yh) * z + at_z) * cores + core) * rows + k
    group_rows = place.shape[0] // groups
    before = jnp.arange(seq_count)[:, None] < jnp.arange(seq_count)[None, :]
    starts = jnp.sum(jnp.where(before[None], lengths[:, :, None], 0), axis=1)
    inside = (
        (at_grp[:, None, None] == jnp.arange(groups)[None, :, None])
        & (place[:, None, None] >= starts[None])
        & (place[:, None, None] < (starts + lengths)[None])
    )
    row_length = jnp.sum(jnp.where(inside, lengths[None].astype(F32), F32(0.0)), axis=(1, 2))
    return (group_rows / seq_count / row_length).reshape(1, -1)


def column(line):
    return jnp.broadcast_to(line, (128, line.shape[1])).T[:, :1]


def share_kernel(
    first_ref, mine_ref, other_ref, items_ref,
    own_grad_ref, other_grad_ref, own_rows_ref, other_rows_ref, log_ref, place_ref, states_ref,
    scores, places, grad, picked,
):
    rows = mine_ref.shape[0] - 1
    chips = mine_ref.shape[1]
    count, width = states_ref.shape
    items = items_ref.shape[0]
    part = count // 2
    block = min(BLOCK, items)
    lanes = min(128, block)
    for half, ref in enumerate((mine_ref, other_ref)):
        digits = ref[rows].astype(F32)
        across = digits.T
        for k in range(rows):
            at = half * part + k * chips
            states_ref[at : at + chips, :] = ref[k]
            found = [digits[:, j * rows + k : j * rows + k + 1].astype(jnp.int32) for j in range(3)]
            found = found[0] + DIGIT * found[1] + DIGIT**2 * found[2] - first_ref[0]
            places[at : at + chips, :] = jnp.broadcast_to(found, (chips, lanes))
            found = [across[j * rows + k : j * rows + k + 1, :].astype(jnp.int32) for j in range(3)]
            found = found[0] + DIGIT * found[1] + DIGIT**2 * found[2] - first_ref[0]
            place_ref[:, at : at + chips] = found
    states = states_ref[...]
    high = None
    for at in range(0, items, block):
        found = lax.dot_general(
            states, items_ref[at : at + block, :], (((1,), (1,)), ((), ())), preferred_element_type=F32
        )
        scores[:, at : at + block] = found
        for c in range(0, block, lanes):
            top = found[:, c : c + lanes]
            high = top if high is None else jnp.maximum(high, top)
    high = jnp.max(high, axis=1, keepdims=True)
    total = None
    lane = lax.broadcasted_iota(jnp.int32, (count, lanes), 1)
    for at in range(0, items, block):
        others, hot = [], []
        for c in range(at, at + block, lanes):
            parts = jnp.exp(scores[:, c : c + lanes] - high)
            total = parts if total is None else total + parts
            matched = places[...] == lane + c
            others.append(jnp.where(matched, 0.0, parts).astype(BF16))
            hot.append(jnp.where(matched, 1.0, 0.0).astype(BF16))
        table = items_ref[at : at + block, :]
        more = jnp.dot(jnp.concatenate(others, axis=1), table, preferred_element_type=F32)
        grad[...] = more if at == 0 else grad[...] + more
        more = jnp.dot(jnp.concatenate(hot, axis=1), table, preferred_element_type=F32)
        picked[...] = more if at == 0 else picked[...] + more
    log_sum = high + jnp.log(jnp.sum(total, axis=1, keepdims=True))
    log_ref[...] = jnp.broadcast_to(log_sum, (count, 128)).T[:1, :]
    share = grad[...] * jnp.exp(high - log_sum)
    own_grad_ref[...] = share[:part]
    other_grad_ref[...] = share[part:]
    own_rows_ref[...] = picked[:part, :].astype(BF16)
    other_rows_ref[...] = picked[part:, :].astype(BF16)


def in_vmem(count):
    return [pl.BlockSpec(memory_space=pltpu.VMEM) for _ in range(count)]


def shares(first, mine, other, items):
    rows, chips, width = mine.shape
    part = (rows - 1) * chips
    count = 2 * part
    return pl.pallas_call(
        share_kernel,
        name="shares",
        out_shape=(
            jax.ShapeDtypeStruct((part, width), F32),
            jax.ShapeDtypeStruct((part, width), F32),
            jax.ShapeDtypeStruct((part, width), BF16),
            jax.ShapeDtypeStruct((part, width), BF16),
            jax.ShapeDtypeStruct((1, count), F32),
            jax.ShapeDtypeStruct((1, count), jnp.int32),
            jax.ShapeDtypeStruct((count, width), BF16),
        ),
        in_specs=[pl.BlockSpec(memory_space=pltpu.SMEM), *in_vmem(3)],
        out_specs=in_vmem(7),
        scratch_shapes=[
            pltpu.VMEM((count, items.shape[0]), F32),
            pltpu.VMEM((count, min(128, items.shape[0])), jnp.int32),
            pltpu.VMEM((count, width), F32),
            pltpu.VMEM((count, width), F32),
        ],
        compiler_params=pltpu.CompilerParams(vmem_limit_bytes=VMEM_LIMIT),
    )(first, mine, other, items)


def three_parts(x):
    high = x.astype(BF16).astype(F32)
    rest = x - high
    middle = rest.astype(BF16).astype(F32)
    return [high, middle, rest - middle]


def pack_kernel(rows, own_grad_ref, other_grad_ref, own_rows_ref, other_rows_ref, own_log_ref, other_log_ref, out_ref):
    length, _, width = out_ref.shape
    part = own_grad_ref.shape[0]
    own = own_log_ref[...]
    other = jnp.concatenate([other_log_ref[:, part:], other_log_ref[:, :part]], axis=1)
    top = jnp.maximum(own, other)
    both = top + jnp.log(jnp.exp(own - top) + jnp.exp(other - top))
    grad = own_grad_ref[...] * column(jnp.exp(own - both)[:, :part])
    grad += other_grad_ref[...] * column(jnp.exp(other - both)[:, :part])
    picked = own_rows_ref[...].astype(F32) + other_rows_ref[...].astype(F32)
    lines = [
        piece[:, at : at + width] for piece in three_parts(both) for at in range(0, 2 * part, width)
    ]
    lines = jnp.concatenate(lines + [jnp.zeros((-len(lines) % 8, width), F32)])
    across = lambda x: [
        x.reshape(rows, length, -1, width)[k] for k in range(rows)
    ]
    sent = across(grad) + across(picked) + [jnp.broadcast_to(lines[None], (length, *lines.shape))]
    out_ref[...] = jnp.concatenate(sent, axis=1).astype(BF16)


def packed(rows, length, *pieces):
    part, width = pieces[0].shape
    lines = 3 * 2 * part // width
    height = 2 * (part // length) + lines + -lines % 8
    return pl.pallas_call(
        functools.partial(pack_kernel, rows),
        name="packed",
        out_shape=jax.ShapeDtypeStruct((length, height, width), BF16),
        in_specs=in_vmem(6),
        out_specs=pl.BlockSpec(memory_space=pltpu.VMEM),
        compiler_params=pltpu.CompilerParams(vmem_limit_bytes=VMEM_LIMIT),
    )(*pieces)


def table_kernel(place_ref, log_ref, weight_ref, states_ref, items_ref, out_ref, *scratch):
    buffers, sems = scratch
    items = items_ref.shape[0]
    block = min(BLOCK, items)
    copies = []
    for step, at in enumerate(range(0, items, block)):
        scores = lax.dot_general(
            items_ref[at : at + block, :], states_ref[...], (((1,), (1,)), ((), ())),
            preferred_element_type=F32,
        )
        parts = jnp.exp(scores - log_ref[...])
        matched = lax.broadcasted_iota(jnp.int32, parts.shape, 0) == place_ref[...] - at
        signal = (weight_ref[...] * jnp.where(matched, parts - 1.0, parts)).astype(BF16)
        buffers[at : at + block, :] = jnp.dot(
            signal, states_ref[...], preferred_element_type=F32
        ).astype(BF16)
        copies.append(
            pltpu.make_async_copy(
                buffers.at[pl.ds(at, block)], out_ref.at[pl.ds(at, block)], sems.at[step]
            )
        )
        copies[-1].start()
    for copy in copies:
        copy.wait()


def table_gradient(place, log_total, weight, states, items):
    return pl.pallas_call(
        table_kernel,
        name="table_gradient",
        out_shape=jax.ShapeDtypeStruct(items.shape, BF16),
        in_specs=in_vmem(5),
        out_specs=pl.BlockSpec(memory_space=pl.ANY),
        scratch_shapes=[
            pltpu.VMEM(items.shape, BF16),
            pltpu.SemaphoreType.DMA((items.shape[0] // min(BLOCK, items.shape[0]),)),
        ],
        compiler_params=pltpu.CompilerParams(vmem_limit_bytes=VMEM_LIMIT),
    )(place, log_total, weight, states, items)


def thirds(x):
    high = lax.reduce_precision(x, 8, 7)
    rest = x - high
    middle = lax.reduce_precision(rest, 8, 7)
    return jnp.concatenate([high, middle, rest - middle]).astype(BF16)


def merged_logs(parts):
    top = jnp.max(parts, axis=0)
    return top + jnp.log(jnp.sum(jnp.exp(parts - top[None]), axis=0))


def merged(arrived, kept, count, own):
    length, _, width = arrived.shape
    given = arrived[:, 2 * kept : 2 * kept + 3 * count // width]
    given = given.astype(F32).reshape(length, 3, count).sum(axis=1)
    logs = merged_logs(given)
    scale = jnp.exp(own(given) - own(logs[None]))
    grad = jnp.sum(arrived[:, :kept].astype(F32) * scale[:, :, None], axis=0)
    picked = jnp.sum(arrived[:, kept : 2 * kept].astype(F32), axis=0)
    return grad, picked, logs


def local(hidden, item_table, targets, lengths):
    rows, width = hidden.shape
    group = lax.axis_index("grp")
    own_items = item_table.shape[0] // 2
    items = lax.dynamic_slice_in_dim(item_table, group * own_items, own_items)
    first_own = (lax.axis_index(ITEM) * 2 + group) * own_items
    plane, depth = lax.axis_size(PLANE), lax.axis_size("z")
    weight = weights_for(lengths, rows)
    mine, other = gathered(hidden, targets)
    own_grad, other_grad, own_picked, other_picked, logs, place, states = shares(
        first_own.reshape(1).astype(jnp.int32), mine, other, items
    )
    count = states.shape[0]
    sent = packed(
        rows, plane, own_grad, from_pair(other_grad), own_picked, from_pair(other_picked),
        logs, from_pair(logs),
    )
    arrived = lax.all_to_all(sent, PLANE, 0, 0, tiled=True)
    in_plane = lambda x: lax.dynamic_index_in_dim(
        x.reshape(x.shape[0], 2, rows, plane, depth)[:, 0], lax.axis_index(PLANE), 2, False
    )
    grad, picked, logs = merged(
        arrived, rows * depth, count, lambda x: in_plane(x).reshape(x.shape[0], -1)
    )
    by_depth = lambda x: jnp.swapaxes(x.reshape(rows, depth, width), 0, 1).astype(BF16)
    lines = thirds(logs).reshape(-1, width)
    lines = jnp.broadcast_to(lines[None], (depth, *lines.shape))
    sent = jnp.concatenate([by_depth(grad), by_depth(picked), lines], axis=1)
    arrived = lax.all_to_all(sent, "z", 0, 0, tiled=True)
    own = lambda x: lax.dynamic_index_in_dim(in_plane(x), lax.axis_index("z"), 2, False)
    grad, picked, logs = merged(arrived, rows, count, own)
    own_logs = own(logs[None])[0]
    own_weight = own(weight)[0]
    target_score = jnp.sum(hidden.astype(F32) * picked, axis=1)
    row_loss = own_logs - target_score
    pull = lax.reduce_precision(own_weight * (jnp.exp(target_score - own_logs) - 1.0), 8, 7)
    hidden_grad = (own_weight[:, None] * grad + pull[:, None] * picked).astype(BF16)
    table_grad = table_gradient(place, logs[None], weight, states, items)
    return (row_loss, hidden_grad, table_grad)


def mapped(split):
    return jax.shard_map(
        local,
        mesh=split,
        in_specs=(P(GRP_ITEM, None), P(ITEM, None), P(GRP_ITEM), P()),
        out_specs=(P(GRP_ITEM), P(GRP_ITEM, None), P(ITEM_GRP, None)),
        check_vma=False,
    )


def solution(mesh):
    return mapped(
        Mesh(
            mesh.devices.reshape(4, 2, 8, 2, mesh.shape["grp"]),
            ("x", "yh", "z", "core", "grp"),
        )
    )
```

```python
import jax
import jax.numpy as jnp
from jax import lax
from jax.experimental import pallas as pl
from jax.experimental.pallas import tpu as pltpu
from jax.sharding import Mesh
from jax.sharding import PartitionSpec as P

ITEM = ("x", "yh", "z", "core")
GRP_ITEM = ("grp", "x", "yh", "z", "core")
ITEM_GRP = ("x", "yh", "z", "core", "grp")
PLANE = ("x", "yh", "grp")
CHIPS = ("x", "yh", "grp", "z")
DIGIT = 128
BLOCK = 512
MIB = 1 << 20
F32 = jnp.float32
BF16 = jnp.bfloat16


def from_pair(x):
    return lax.ppermute(x, "core", [(0, 1), (1, 0)])


def spread_kernel(targets_ref, hidden_ref, out_ref):
    _, height, width = out_ref.shape
    rows = height - 1
    lane = lax.broadcasted_iota(jnp.int32, (1, width), 1)
    digits = jnp.zeros((1, width), jnp.int32)
    for k in range(rows):
        rest = targets_ref[k]
        for j in range(3):
            digits = jnp.where(lane == j * rows + k, rest % DIGIT, digits)
            rest = rest // DIGIT
    line = jnp.concatenate([hidden_ref[...].astype(F32), digits.astype(F32)])
    out_ref[...] = jnp.broadcast_to(line[None], out_ref.shape).astype(BF16)


def spread(hidden, targets, chips):
    rows, width = hidden.shape
    return pl.pallas_call(
        spread_kernel,
        name="spread",
        out_shape=jax.ShapeDtypeStruct((chips, rows + 1, width), BF16),
        in_specs=[pl.BlockSpec(memory_space=pltpu.SMEM), *in_vmem(1)],
        out_specs=pl.BlockSpec(memory_space=pltpu.VMEM),
        compiler_params=pltpu.CompilerParams(vmem_limit_bytes=4 * MIB),
    )(targets, hidden)


def in_vmem(count):
    return [pl.BlockSpec(memory_space=pltpu.VMEM) for _ in range(count)]


def weights_for(lengths, rows):
    groups, seq_count = lengths.shape
    cores, x, yh, grps, z = (lax.axis_size(axis) for axis in ("core", "x", "yh", "grp", "z"))
    half, k, at_x, at_yh, at_grp, at_z = jnp.unravel_index(
        jnp.arange(cores * rows * x * yh * grps * z), (cores, rows, x, yh, grps, z)
    )
    core = (half + lax.axis_index("core")) % cores
    place = (((at_x * yh + at_yh) * z + at_z) * cores + core) * rows + k
    group_rows = place.shape[0] // groups
    before = jnp.arange(seq_count)[:, None] < jnp.arange(seq_count)[None, :]
    starts = jnp.sum(jnp.where(before[None], lengths[:, :, None], 0), axis=1)
    inside = (
        (at_grp[:, None, None] == jnp.arange(groups)[None, :, None])
        & (place[:, None, None] >= starts[None])
        & (place[:, None, None] < (starts + lengths)[None])
    )
    row_length = jnp.sum(jnp.where(inside, lengths[None].astype(F32), F32(0.0)), axis=(1, 2))
    return (group_rows / seq_count / row_length).reshape(1, -1)


def column(line):
    return jnp.broadcast_to(line, (128, line.shape[1])).T[:, :1]


def share_kernel(
    first_ref, mine_ref, other_ref, items_ref,
    own_grad_ref, other_grad_ref, own_rows_ref, other_rows_ref, log_ref, place_ref, states_ref,
    scores, places, grad, picked,
):
    rows = mine_ref.shape[0] - 1
    chips = mine_ref.shape[1]
    count, _ = states_ref.shape
    items = items_ref.shape[0]
    part = count // 2
    block = min(BLOCK, items)
    lanes = min(128, block)
    for half, ref in enumerate((mine_ref, other_ref)):
        digits = ref[rows].astype(F32)
        across = digits.T
        for k in range(rows):
            at = half * part + k * chips
            states_ref[at : at + chips, :] = ref[k]
            found = [digits[:, j * rows + k : j * rows + k + 1].astype(jnp.int32) for j in range(3)]
            found = found[0] + DIGIT * found[1] + DIGIT**2 * found[2] - first_ref[0]
            places[at : at + chips, :] = jnp.broadcast_to(found, (chips, lanes))
            found = [across[j * rows + k : j * rows + k + 1, :].astype(jnp.int32) for j in range(3)]
            found = found[0] + DIGIT * found[1] + DIGIT**2 * found[2] - first_ref[0]
            place_ref[:, at : at + chips] = found
    states = states_ref[...]
    high = None
    for at in range(0, items, block):
        found = lax.dot_general(
            states, items_ref[at : at + block, :], (((1,), (1,)), ((), ())), preferred_element_type=F32
        )
        scores[:, at : at + block] = found
        for c in range(0, block, lanes):
            top = found[:, c : c + lanes]
            high = top if high is None else jnp.maximum(high, top)
    high = jnp.max(high, axis=1, keepdims=True)
    total = None
    lane = lax.broadcasted_iota(jnp.int32, (count, lanes), 1)
    for at in range(0, items, block):
        others, hot = [], []
        for c in range(at, at + block, lanes):
            parts = jnp.exp(scores[:, c : c + lanes] - high)
            total = parts if total is None else total + parts
            matched = places[...] == lane + c
            others.append(jnp.where(matched, 0.0, parts).astype(BF16))
            hot.append(jnp.where(matched, 1.0, 0.0).astype(BF16))
        table = items_ref[at : at + block, :]
        more = jnp.dot(jnp.concatenate(others, axis=1), table, preferred_element_type=F32)
        grad[...] = more if at == 0 else grad[...] + more
        more = jnp.dot(jnp.concatenate(hot, axis=1), table, preferred_element_type=F32)
        picked[...] = more if at == 0 else picked[...] + more
    log_sum = high + jnp.log(jnp.sum(total, axis=1, keepdims=True))
    log_ref[...] = jnp.broadcast_to(log_sum, (count, 128)).T[:1, :]
    share = grad[...] * jnp.exp(high - log_sum)
    own_grad_ref[...] = share[:part]
    other_grad_ref[...] = share[part:]
    own_rows_ref[...] = picked[:part, :].astype(BF16)
    other_rows_ref[...] = picked[part:, :].astype(BF16)


def shares(first, mine, other, items):
    rows, chips, width = mine.shape
    part = (rows - 1) * chips
    count = 2 * part
    return pl.pallas_call(
        share_kernel,
        name="shares",
        out_shape=(
            jax.ShapeDtypeStruct((part, width), F32),
            jax.ShapeDtypeStruct((part, width), F32),
            jax.ShapeDtypeStruct((part, width), BF16),
            jax.ShapeDtypeStruct((part, width), BF16),
            jax.ShapeDtypeStruct((1, count), F32),
            jax.ShapeDtypeStruct((1, count), jnp.int32),
            jax.ShapeDtypeStruct((count, width), BF16),
        ),
        in_specs=[pl.BlockSpec(memory_space=pltpu.SMEM), *in_vmem(3)],
        out_specs=in_vmem(7),
        scratch_shapes=[
            pltpu.VMEM((count, items.shape[0]), F32),
            pltpu.VMEM((count, min(128, items.shape[0])), jnp.int32),
            pltpu.VMEM((count, width), F32),
            pltpu.VMEM((count, width), F32),
        ],
        compiler_params=pltpu.CompilerParams(vmem_limit_bytes=32 * MIB),
    )(first, mine, other, items)


def three_parts(x):
    high = x.astype(BF16).astype(F32)
    rest = x - high
    middle = rest.astype(BF16).astype(F32)
    return [high, middle, rest - middle]


def swapped(x):
    part = x.shape[1] // 2
    return jnp.concatenate([x[:, part:], x[:, :part]], axis=1)


def swapped(x):
    part = x.shape[1] // 2
    return jnp.concatenate([x[:, part:], x[:, :part]], axis=1)


def pack_kernel(rows, own_grad_ref, other_grad_ref, own_rows_ref, other_rows_ref, own_log_ref, other_log_ref, out_ref):
    length, _, width = out_ref.shape
    part = own_grad_ref.shape[0]
    own = own_log_ref[...]
    other = swapped(other_log_ref[...])
    top = jnp.maximum(own, other)
    both = top + jnp.log(jnp.exp(own - top) + jnp.exp(other - top))
    grad = own_grad_ref[...] * column(jnp.exp(own - both)[:, :part])
    grad += other_grad_ref[...] * column(jnp.exp(other - both)[:, :part])
    picked = own_rows_ref[...].astype(F32) + other_rows_ref[...].astype(F32)
    lines = [
        piece[:, at : at + width] for piece in three_parts(both) for at in range(0, 2 * part, width)
    ]
    lines = jnp.concatenate(lines + [jnp.zeros((-len(lines) % 8, width), F32)])
    across = lambda x: [
        x.reshape(rows, length, -1, width)[k] for k in range(rows)
    ]
    sent = across(grad) + across(picked) + [jnp.broadcast_to(lines[None], (length, *lines.shape))]
    out_ref[...] = jnp.concatenate(sent, axis=1).astype(BF16)


def packed(rows, length, *pieces):
    part, width = pieces[0].shape
    lines = 3 * 2 * part // width
    height = 2 * (part // length) + lines + -lines % 8
    return pl.pallas_call(
        lambda *refs: pack_kernel(rows, *refs),
        name="packed",
        out_shape=jax.ShapeDtypeStruct((length, height, width), BF16),
        in_specs=in_vmem(6),
        out_specs=pl.BlockSpec(memory_space=pltpu.VMEM),
        compiler_params=pltpu.CompilerParams(vmem_limit_bytes=12 * MIB),
    )(*pieces)


def merged(arrived_ref, at, wide):
    lines = arrived_ref[...].astype(F32)
    parts = sum(lines[:, at + j * wide : at + (j + 1) * wide] for j in range(3))
    top = jnp.max(parts, axis=0)
    logs = top + jnp.log(jnp.sum(jnp.exp(parts - top[None]), axis=0))
    return lines, jnp.exp(parts - logs[None]), logs


def middle_kernel(rows, plane_ref, arrived_ref, out_ref, turned, built):
    length = arrived_ref.shape[0]
    depth, height, width = out_ref.shape
    chips = length * depth
    wide = 2 * rows * chips // width
    kept = rows * depth
    lines, scale, logs = merged(arrived_ref, 2 * kept, wide)
    scale = scale.reshape(length * wide, width)
    pad = jnp.zeros((-(length * wide) % 128, width), F32)
    turned[...] = jnp.concatenate([scale, pad]).T
    for k in range(rows):
        c, lane = k * chips // width, k * chips % width
        across = turned[pl.ds(pl.multiple_of(plane_ref[0] * depth + lane, depth), depth), :]
        grad = jnp.zeros((depth, width), F32)
        picked = jnp.zeros((depth, width), F32)
        for j in range(length):
            at = j * wide + c
            grad += lines[j, k * depth : (k + 1) * depth] * across[:, at : at + 1]
            picked += lines[j, kept + k * depth : kept + (k + 1) * depth]
        for z in range(depth):
            built[z, k : k + 1, :] = grad[z : z + 1]
            built[z, rows + k : rows + k + 1, :] = picked[z : z + 1]
    lines = jnp.concatenate(three_parts(logs))
    at = 2 * rows
    built[:, at : at + 3 * wide, :] = jnp.broadcast_to(lines[None], (depth, 3 * wide, width))
    at += 3 * wide
    if height > at:
        built[:, at:, :] = jnp.zeros((depth, height - at, width), F32)
    out_ref[...] = built[...].astype(BF16)


def middle(rows, depth, plane, arrived):
    length, _, width = arrived.shape
    wide = 2 * rows * length * depth // width
    height = 2 * rows + 3 * wide
    height += -height % 8
    return pl.pallas_call(
        lambda *refs: middle_kernel(rows, *refs),
        name="middle",
        out_shape=jax.ShapeDtypeStruct((depth, height, width), BF16),
        in_specs=[pl.BlockSpec(memory_space=pltpu.SMEM), *in_vmem(1)],
        out_specs=pl.BlockSpec(memory_space=pltpu.VMEM),
        scratch_shapes=[
            pltpu.VMEM((width, length * wide + -(length * wide) % 128), F32),
            pltpu.VMEM((depth, height, width), F32),
        ],
        compiler_params=pltpu.CompilerParams(vmem_limit_bytes=12 * MIB),
    )(plane, arrived)


def last_kernel(
    chip_ref, arrived_ref, place_ref, weight_ref, hidden_ref, states_ref, items_ref,
    loss_ref, hidden_grad_ref, table_grad_ref, buffer, sems,
):
    rows, width = hidden_ref.shape
    depth = arrived_ref.shape[0]
    items = items_ref.shape[0]
    count = states_ref.shape[0]
    block = min(BLOCK, items)
    chips = count // (2 * rows)
    wide = count // width
    lines, scale, logs = merged(arrived_ref, 2 * rows, wide)
    line = jnp.concatenate([logs[c : c + 1] for c in range(wide)], axis=1)
    weight = weight_ref[...]
    states = states_ref[...]
    copies = []
    for step, at in enumerate(range(0, items, block)):
        scores = lax.dot_general(
            items_ref[at : at + block, :], states, (((1,), (1,)), ((), ())),
            preferred_element_type=F32,
        )
        parts = jnp.exp(scores - line)
        matched = lax.broadcasted_iota(jnp.int32, parts.shape, 0) == place_ref[...] - at
        signal = (weight * jnp.where(matched, parts - 1.0, parts)).astype(BF16)
        buffer[at : at + block, :] = jnp.dot(
            signal, states, preferred_element_type=F32
        ).astype(BF16)
        copies.append(
            pltpu.make_async_copy(
                buffer.at[pl.ds(at, block)], table_grad_ref.at[pl.ds(at, block)], sems.at[step]
            )
        )
        copies[-1].start()
    lane = lax.broadcasted_iota(jnp.int32, (1, width), 1)
    hidden = hidden_ref[...].astype(F32)
    place = lax.broadcasted_iota(jnp.int32, loss_ref.shape, 1)
    losses = jnp.zeros(loss_ref.shape, F32)
    grads = []
    for k in range(rows):
        c, first = k * chips // width, k * chips % width
        mine = lambda x: jnp.sum(
            jnp.where(lane == chip_ref[0] + first, x, 0.0), axis=1, keepdims=True
        )
        log_total = mine(logs[c : c + 1])
        own_weight = mine(weight[:, c * width : (c + 1) * width])
        grad = jnp.zeros((1, width), F32)
        picked = jnp.zeros((1, width), F32)
        for j in range(depth):
            grad += lines[j, k : k + 1] * mine(scale[j, c : c + 1])
            picked += lines[j, rows + k : rows + k + 1]
        score = jnp.sum(hidden[k : k + 1] * picked, axis=1, keepdims=True)
        losses = jnp.where(place == k, log_total - score, losses)
        pull = (own_weight * (jnp.exp(score - log_total) - 1.0)).astype(BF16).astype(F32)
        grads.append(own_weight * grad + pull * picked)
    loss_ref[...] = losses
    hidden_grad_ref[...] = jnp.concatenate(grads).astype(BF16)
    for copy in copies:
        copy.wait()


def last(chip, arrived, place, weight, hidden, states, items):
    rows, width = hidden.shape
    return pl.pallas_call(
        last_kernel,
        name="last",
        out_shape=(
            jax.ShapeDtypeStruct((1, rows), F32),
            jax.ShapeDtypeStruct((rows, width), BF16),
            jax.ShapeDtypeStruct(items.shape, BF16),
        ),
        in_specs=[pl.BlockSpec(memory_space=pltpu.SMEM), *in_vmem(6)],
        out_specs=[*in_vmem(2), pl.BlockSpec(memory_space=pl.ANY)],
        scratch_shapes=[
            pltpu.VMEM(items.shape, BF16),
            pltpu.SemaphoreType.DMA((items.shape[0] // min(BLOCK, items.shape[0]),)),
        ],
        compiler_params=pltpu.CompilerParams(vmem_limit_bytes=16 * MIB),
    )(chip, arrived, place, weight, hidden, states, items)


def steps(hidden, item_table, targets, lengths):
    rows, _ = hidden.shape
    group = lax.axis_index("grp")
    chip = lax.axis_index(CHIPS).reshape(1)
    own_items = item_table.shape[0] // 2
    items = lax.dynamic_slice_in_dim(item_table, group * own_items, own_items)
    first_own = (lax.axis_index(ITEM) * 2 + group) * own_items
    weight = weights_for(lengths, rows)
    sent = spread(hidden, targets, lax.axis_size(CHIPS))
    mine = lax.all_to_all(sent, CHIPS, 0, 0, tiled=True)
    mine = jnp.swapaxes(mine, 0, 1)
    own_grad, other_grad, own_picked, other_picked, logs, place, states = shares(
        first_own.reshape(1), mine, from_pair(mine), items
    )
    sent = packed(
        rows, lax.axis_size(PLANE), own_grad, from_pair(other_grad), own_picked,
        from_pair(other_picked), logs, from_pair(logs),
    )
    arrived = lax.all_to_all(sent, PLANE, 0, 0, tiled=True)
    sent = middle(rows, lax.axis_size("z"), lax.axis_index(PLANE).reshape(1), arrived)
    arrived = lax.all_to_all(sent, "z", 0, 0, tiled=True)
    row_loss, hidden_grad, table_grad = last(
        chip, arrived, place, weight, hidden, states, items
    )
    return (row_loss.reshape(-1), hidden_grad, table_grad)


def mapped(split):
    return jax.shard_map(
        steps,
        mesh=split,
        in_specs=(P(GRP_ITEM, None), P(ITEM, None), P(GRP_ITEM), P()),
        out_specs=(P(GRP_ITEM), P(GRP_ITEM, None), P(ITEM_GRP, None)),
        check_vma=False,
    )


def solution(mesh):
    split = Mesh(
        mesh.devices.reshape(4, 2, 8, 2, mesh.shape["grp"]),
        ("x", "yh", "z", "core", "grp"),
    )
    return mapped(split)
```

```python
import jax
import jax.numpy as jnp
from jax import lax
from jax.experimental import pallas as pl
from jax.experimental.pallas import tpu as pltpu
from jax.sharding import Mesh
from jax.sharding import PartitionSpec as P

ITEM = ("x", "yh", "z", "core")
GRP_ITEM = ("grp", "x", "yh", "z", "core")
ITEM_GRP = ("x", "yh", "z", "core", "grp")
PLANE = ("x", "yh", "grp")
CHIPS = ("x", "yh", "grp", "z")
DIGIT = 128
BLOCK = 512
MIB = 1 << 20
F32 = jnp.float32
BF16 = jnp.bfloat16


def from_pair(x):
    return lax.ppermute(x, "core", [(0, 1), (1, 0)])


def spread_kernel(targets_hbm, hidden_hbm, out_ref, targets_ref, hidden_ref, sems):
    copies = [
        pltpu.make_async_copy(targets_hbm, targets_ref, sems.at[0]),
        pltpu.make_async_copy(hidden_hbm, hidden_ref, sems.at[1]),
    ]
    for copy in copies:
        copy.start()
    for copy in copies:
        copy.wait()
    _, height, width = out_ref.shape
    rows = height - 1
    lane = lax.broadcasted_iota(jnp.int32, (1, width), 1)
    digits = jnp.zeros((1, width), jnp.int32)
    for k in range(rows):
        rest = targets_ref[k]
        for j in range(3):
            digits = jnp.where(lane == j * rows + k, rest % DIGIT, digits)
            rest = rest // DIGIT
    line = jnp.concatenate([hidden_ref[...].astype(F32), digits.astype(F32)])
    out_ref[...] = jnp.broadcast_to(line[None], out_ref.shape).astype(BF16)


def spread(hidden, targets, chips):
    rows, width = hidden.shape
    return pl.pallas_call(
        spread_kernel,
        name="spread",
        out_shape=jax.ShapeDtypeStruct((chips, rows + 1, width), BF16),
        in_specs=[pl.BlockSpec(memory_space=pltpu.HBM)] * 2,
        out_specs=pl.BlockSpec(memory_space=pltpu.VMEM),
        scratch_shapes=[
            pltpu.SMEM(targets.shape, jnp.int32),
            pltpu.VMEM(hidden.shape, BF16),
            pltpu.SemaphoreType.DMA((2,)),
        ],
        compiler_params=pltpu.CompilerParams(vmem_limit_bytes=4 * MIB),
    )(in_hbm(targets), in_hbm(hidden))


def in_hbm(x):
    return pltpu.with_memory_space_constraint(x, pltpu.HBM)


def in_vmem(count):
    return [pl.BlockSpec(memory_space=pltpu.VMEM) for _ in range(count)]


def weights_for(lengths, rows):
    groups, seq_count = lengths.shape
    cores, x, yh, grps, z = (lax.axis_size(axis) for axis in ("core", "x", "yh", "grp", "z"))
    half, k, at_x, at_yh, at_grp, at_z = jnp.unravel_index(
        jnp.arange(cores * rows * x * yh * grps * z), (cores, rows, x, yh, grps, z)
    )
    core = (half + lax.axis_index("core")) % cores
    place = (((at_x * yh + at_yh) * z + at_z) * cores + core) * rows + k
    group_rows = place.shape[0] // groups
    before = jnp.arange(seq_count)[:, None] < jnp.arange(seq_count)[None, :]
    starts = jnp.sum(jnp.where(before[None], lengths[:, :, None], 0), axis=1)
    inside = (
        (at_grp[:, None, None] == jnp.arange(groups)[None, :, None])
        & (place[:, None, None] >= starts[None])
        & (place[:, None, None] < (starts + lengths)[None])
    )
    row_length = jnp.sum(jnp.where(inside, lengths[None].astype(F32), F32(0.0)), axis=(1, 2))
    return (group_rows / seq_count / row_length).reshape(1, -1)


def column(line):
    return jnp.broadcast_to(line, (128, line.shape[1])).T[:, :1]


def share_kernel(
    first_ref, given_ref, items_ref, grad_ref, rows_ref, log_ref, place_ref, states_ref,
    scores, places, grad, picked,
):
    rows = given_ref.shape[0] - 1
    chips = given_ref.shape[1]
    count, _ = states_ref.shape
    items = items_ref.shape[0]
    block = min(BLOCK, items)
    lanes = min(128, block)
    digits = given_ref[rows].astype(F32)
    across = digits.T
    for k in range(rows):
        at = k * chips
        states_ref[at : at + chips, :] = given_ref[k]
        found = [digits[:, j * rows + k : j * rows + k + 1].astype(jnp.int32) for j in range(3)]
        found = found[0] + DIGIT * found[1] + DIGIT**2 * found[2] - first_ref[0]
        places[at : at + chips, :] = jnp.broadcast_to(found, (chips, lanes))
        found = [across[j * rows + k : j * rows + k + 1, :].astype(jnp.int32) for j in range(3)]
        found = found[0] + DIGIT * found[1] + DIGIT**2 * found[2] - first_ref[0]
        place_ref[:, at : at + chips] = found
    states = states_ref[...]
    high = None
    for at in range(0, items, block):
        found = lax.dot_general(
            states, items_ref[at : at + block, :], (((1,), (1,)), ((), ())), preferred_element_type=F32
        )
        scores[:, at : at + block] = found
        for c in range(0, block, lanes):
            top = found[:, c : c + lanes]
            high = top if high is None else jnp.maximum(high, top)
    high = jnp.max(high, axis=1, keepdims=True)
    total = None
    lane = lax.broadcasted_iota(jnp.int32, (1, lanes), 1)
    for at in range(0, items, block):
        others, hot = [], []
        for c in range(at, at + block, lanes):
            parts = jnp.exp(scores[:, c : c + lanes] - high)
            total = parts if total is None else total + parts
            matched = places[...] == lane + c
            others.append(jnp.where(matched, 0.0, parts).astype(BF16))
            hot.append(jnp.where(matched, 1.0, 0.0).astype(BF16))
        table = items_ref[at : at + block, :]
        more = jnp.dot(jnp.concatenate(others, axis=1), table, preferred_element_type=F32)
        grad[...] = more if at == 0 else grad[...] + more
        more = jnp.dot(jnp.concatenate(hot, axis=1), table, preferred_element_type=F32)
        picked[...] = more if at == 0 else picked[...] + more
    log_sum = high + jnp.log(jnp.sum(total, axis=1, keepdims=True))
    log_ref[...] = jnp.broadcast_to(log_sum, (count, 128)).T[:1, :]
    grad_ref[...] = grad[...] * jnp.exp(high - log_sum)
    rows_ref[...] = picked[...].astype(BF16)


def shares(first, given, items):
    height, chips, width = given.shape
    count = (height - 1) * chips
    return pl.pallas_call(
        share_kernel,
        name="shares",
        out_shape=(
            jax.ShapeDtypeStruct((count, width), F32),
            jax.ShapeDtypeStruct((count, width), BF16),
            jax.ShapeDtypeStruct((1, count), F32),
            jax.ShapeDtypeStruct((1, count), jnp.int32),
            jax.ShapeDtypeStruct((count, width), BF16),
        ),
        in_specs=[pl.BlockSpec(memory_space=pltpu.SMEM), *in_vmem(2)],
        out_specs=in_vmem(5),
        scratch_shapes=[
            pltpu.VMEM((count, items.shape[0]), F32),
            pltpu.VMEM((count, min(128, BLOCK)), jnp.int32),
            pltpu.VMEM((count, width), F32),
            pltpu.VMEM((count, width), F32),
        ],
        compiler_params=pltpu.CompilerParams(vmem_limit_bytes=24 * MIB),
    )(first, given, items)


def three_parts(x):
    high = x.astype(BF16).astype(F32)
    rest = x - high
    middle = rest.astype(BF16).astype(F32)
    return [high, middle, rest - middle]


def pack_kernel(
    rows, own_grad_ref, other_grad_ref, own_rows_ref, other_rows_ref,
    own_log_ref, far_log_ref, other_log_ref, other_far_log_ref, out_ref,
):
    length, _, width = out_ref.shape
    part = own_grad_ref.shape[0]
    own = jnp.concatenate([own_log_ref[...], far_log_ref[...]], axis=1)
    other = jnp.concatenate([other_far_log_ref[...], other_log_ref[...]], axis=1)
    top = jnp.maximum(own, other)
    both = top + jnp.log(jnp.exp(own - top) + jnp.exp(other - top))
    grad = own_grad_ref[...] * column(jnp.exp(own - both)[:, :part])
    grad += other_grad_ref[...] * column(jnp.exp(other - both)[:, :part])
    picked = own_rows_ref[...].astype(F32) + other_rows_ref[...].astype(F32)
    lines = [
        piece[:, at : at + width] for piece in three_parts(both) for at in range(0, 2 * part, width)
    ]
    lines = jnp.concatenate(lines + [jnp.zeros((-len(lines) % 8, width), F32)])
    across = lambda x: [
        x.reshape(rows, length, -1, width)[k] for k in range(rows)
    ]
    sent = across(grad) + across(picked) + [jnp.broadcast_to(lines[None], (length, *lines.shape))]
    out_ref[...] = jnp.concatenate(sent, axis=1).astype(BF16)


def packed(rows, length, *pieces):
    part, width = pieces[0].shape
    lines = 3 * 2 * part // width
    height = 2 * (part // length) + lines + -lines % 8
    return pl.pallas_call(
        lambda *refs: pack_kernel(rows, *refs),
        name="packed",
        out_shape=jax.ShapeDtypeStruct((length, height, width), BF16),
        in_specs=in_vmem(8),
        out_specs=pl.BlockSpec(memory_space=pltpu.VMEM),
        compiler_params=pltpu.CompilerParams(vmem_limit_bytes=12 * MIB),
    )(*pieces)


def merged(arrived_ref, at, wide):
    lines = arrived_ref[...].astype(F32)
    parts = sum(lines[:, at + j * wide : at + (j + 1) * wide] for j in range(3))
    top = jnp.max(parts, axis=0)
    logs = top + jnp.log(jnp.sum(jnp.exp(parts - top[None]), axis=0))
    return lines, jnp.exp(parts - logs[None]), logs


def middle_kernel(rows, plane_ref, arrived_ref, out_ref, turned, built):
    length = arrived_ref.shape[0]
    depth, height, width = out_ref.shape
    chips = length * depth
    wide = 2 * rows * chips // width
    kept = rows * depth
    lines, scale, logs = merged(arrived_ref, 2 * kept, wide)
    scale = scale.reshape(length * wide, width)
    pad = jnp.zeros((-(length * wide) % 128, width), F32)
    turned[...] = jnp.concatenate([scale, pad]).T
    for k in range(rows):
        c, lane = k * chips // width, k * chips % width
        across = turned[pl.ds(pl.multiple_of(plane_ref[0] * depth + lane, depth), depth), :]
        grad = jnp.zeros((depth, width), F32)
        picked = jnp.zeros((depth, width), F32)
        for j in range(length):
            at = j * wide + c
            grad += lines[j, k * depth : (k + 1) * depth] * across[:, at : at + 1]
            picked += lines[j, kept + k * depth : kept + (k + 1) * depth]
        for z in range(depth):
            built[z, k : k + 1, :] = grad[z : z + 1]
            built[z, rows + k : rows + k + 1, :] = picked[z : z + 1]
    lines = jnp.concatenate(three_parts(logs))
    at = 2 * rows
    built[:, at : at + 3 * wide, :] = jnp.broadcast_to(lines[None], (depth, 3 * wide, width))
    at += 3 * wide
    if height > at:
        built[:, at:, :] = jnp.zeros((depth, height - at, width), F32)
    out_ref[...] = built[...].astype(BF16)


def middle(rows, depth, plane, arrived):
    length, _, width = arrived.shape
    wide = 2 * rows * length * depth // width
    height = 2 * rows + 3 * wide
    height += -height % 8
    return pl.pallas_call(
        lambda *refs: middle_kernel(rows, *refs),
        name="middle",
        out_shape=jax.ShapeDtypeStruct((depth, height, width), BF16),
        in_specs=[pl.BlockSpec(memory_space=pltpu.SMEM), *in_vmem(1)],
        out_specs=pl.BlockSpec(memory_space=pltpu.VMEM),
        scratch_shapes=[
            pltpu.VMEM((width, length * wide + -(length * wide) % 128), F32),
            pltpu.VMEM((depth, height, width), F32),
        ],
        compiler_params=pltpu.CompilerParams(vmem_limit_bytes=12 * MIB),
    )(plane, arrived)


def last_kernel(
    chip_ref, arrived_ref, place_ref, far_place_ref, weight_ref, hidden_ref, states_ref,
    far_states_ref, items_ref, loss_hbm, hidden_grad_hbm, table_grad_hbm,
    states, buffer, loss_ref, hidden_grad_ref, sems,
):
    rows, width = hidden_ref.shape
    depth = arrived_ref.shape[0]
    items = items_ref.shape[0]
    count = states.shape[0]
    block = min(BLOCK, items)
    chips = count // (2 * rows)
    wide = count // width
    copies = []

    def send(source, target):
        copies.append(pltpu.make_async_copy(source, target, sems.at[len(copies)]))
        copies[-1].start()

    lines, scale, logs = merged(arrived_ref, 2 * rows, wide)
    weight = weight_ref[...]
    lane = lax.broadcasted_iota(jnp.int32, (1, width), 1)
    hidden = hidden_ref[...].astype(F32)
    place = lax.broadcasted_iota(jnp.int32, loss_ref.shape, 1)
    losses = jnp.zeros(loss_ref.shape, F32)
    grads = []
    for k in range(rows):
        c, first = k * chips // width, k * chips % width
        mine = lambda x: jnp.sum(
            jnp.where(lane == chip_ref[0] + first, x, 0.0), axis=-1, keepdims=True
        )
        log_total = mine(logs[c : c + 1])
        own_weight = mine(weight[:, c * width : (c + 1) * width])
        grad = jnp.zeros((1, width), F32)
        picked = jnp.zeros((1, width), F32)
        for j in range(depth):
            grad += lines[j, k : k + 1] * mine(scale[j, c : c + 1])
            picked += lines[j, rows + k : rows + k + 1]
        score = jnp.sum(hidden[k : k + 1] * picked, axis=1, keepdims=True)
        losses = jnp.where(place == k, log_total - score, losses)
        pull = (own_weight * (jnp.exp(score - log_total) - 1.0)).astype(BF16).astype(F32)
        grads.append(own_weight * grad + pull * picked)
    loss_ref[...] = losses
    send(loss_ref, loss_hbm)
    hidden_grad_ref[...] = jnp.concatenate(grads).astype(BF16)
    send(hidden_grad_ref, hidden_grad_hbm)
    line = jnp.concatenate([logs[c : c + 1] for c in range(wide)], axis=1)
    places = jnp.concatenate([place_ref[...], far_place_ref[...]], axis=1)
    states[: count // 2, :] = states_ref[...]
    states[count // 2 :, :] = far_states_ref[...]
    for at in range(0, items, block):
        scores = lax.dot_general(
            items_ref[at : at + block, :], states[...], (((1,), (1,)), ((), ())),
            preferred_element_type=F32,
        )
        parts = jnp.exp(scores - line)
        matched = lax.broadcasted_iota(jnp.int32, parts.shape, 0) == places - at
        signal = (weight * jnp.where(matched, parts - 1.0, parts)).astype(BF16)
        buffer[at : at + block, :] = jnp.dot(
            signal, states[...], preferred_element_type=F32
        ).astype(BF16)
        send(buffer.at[pl.ds(at, block)], table_grad_hbm.at[pl.ds(at, block)])
    for copy in copies:
        copy.wait()


def last(chip, arrived, place, far_place, weight, hidden, states, far_states, items):
    rows, width = hidden.shape
    return pl.pallas_call(
        last_kernel,
        name="last",
        out_shape=(
            jax.ShapeDtypeStruct((1, rows), F32),
            jax.ShapeDtypeStruct((rows, width), BF16),
            jax.ShapeDtypeStruct(items.shape, BF16),
        ),
        in_specs=[pl.BlockSpec(memory_space=pltpu.SMEM), *in_vmem(8)],
        out_specs=[pl.BlockSpec(memory_space=pltpu.HBM)] * 3,
        scratch_shapes=[
            pltpu.VMEM((2 * states.shape[0], width), BF16),
            pltpu.VMEM(items.shape, BF16),
            pltpu.VMEM((1, rows), F32),
            pltpu.VMEM((rows, width), BF16),
            pltpu.SemaphoreType.DMA((2 + items.shape[0] // min(BLOCK, items.shape[0]),)),
        ],
        compiler_params=pltpu.CompilerParams(vmem_limit_bytes=16 * MIB),
    )(chip, arrived, place, far_place, weight, hidden, states, far_states, items)


def steps(hidden, item_table, targets, lengths):
    rows, _ = hidden.shape
    group = lax.axis_index("grp")
    chip = lax.axis_index(CHIPS).reshape(1)
    own_items = item_table.shape[0] // 2
    items = lax.dynamic_slice_in_dim(item_table, group * own_items, own_items)
    first_own = (lax.axis_index(ITEM) * 2 + group) * own_items
    weight = weights_for(lengths, rows)
    sent = spread(hidden, targets, lax.axis_size(CHIPS))
    mine = lax.all_to_all(sent, CHIPS, 0, 0, tiled=True)
    mine = jnp.swapaxes(mine, 0, 1)
    first_own = first_own.reshape(1)
    other = from_pair(mine)
    own_grad, own_picked, own_logs, place, states = shares(first_own, mine, items)
    far_grad, far_picked, far_logs, far_place, far_states = shares(first_own, other, items)
    sent = packed(
        rows, lax.axis_size(PLANE), own_grad, from_pair(far_grad), own_picked,
        from_pair(far_picked), own_logs, far_logs, from_pair(own_logs), from_pair(far_logs),
    )
    arrived = lax.all_to_all(sent, PLANE, 0, 0, tiled=True)
    sent = middle(rows, lax.axis_size("z"), lax.axis_index(PLANE).reshape(1), arrived)
    arrived = lax.all_to_all(sent, "z", 0, 0, tiled=True)
    row_loss, hidden_grad, table_grad = last(
        chip, arrived, place, far_place, weight, hidden, states, far_states, items
    )
    return (row_loss.reshape(-1), hidden_grad, table_grad)


def mapped(split):
    return jax.shard_map(
        steps,
        mesh=split,
        in_specs=(P(GRP_ITEM, None), P(ITEM, None), P(GRP_ITEM), P()),
        out_specs=(P(GRP_ITEM), P(GRP_ITEM, None), P(ITEM_GRP, None)),
        check_vma=False,
    )


def solution(mesh):
    split = Mesh(
        mesh.devices.reshape(4, 2, 8, 2, mesh.shape["grp"]),
        ("x", "yh", "z", "core", "grp"),
    )
    return mapped(split)
```

```python
import jax
import jax.numpy as jnp
from jax import lax
from jax.experimental import pallas as pl
from jax.experimental.pallas import tpu as pltpu
from jax.sharding import Mesh
from jax.sharding import PartitionSpec as P

ITEM = ("x", "yh", "z", "core")
GRP_ITEM = ("grp", "x", "yh", "z", "core")
ITEM_GRP = ("x", "yh", "z", "core", "grp")
PLANE = ("x", "yh", "grp")
CHIPS = ("x", "yh", "grp", "z")
DIGIT = 128
BLOCK = 512
MIB = 1 << 20
F32 = jnp.float32
BF16 = jnp.bfloat16


def from_pair(x):
    return lax.ppermute(x, "core", [(0, 1), (1, 0)])


def spread_kernel(targets_hbm, hidden_hbm, out_ref, targets_ref, hidden_ref, sems):
    copies = [
        pltpu.make_async_copy(targets_hbm, targets_ref, sems.at[0]),
        pltpu.make_async_copy(hidden_hbm, hidden_ref, sems.at[1]),
    ]
    for copy in copies:
        copy.start()
    for copy in copies:
        copy.wait()
    _, height, width = out_ref.shape
    rows = height - 1
    lane = lax.broadcasted_iota(jnp.int32, (1, width), 1)
    digits = jnp.zeros((1, width), jnp.int32)
    for k in range(rows):
        rest = targets_ref[k]
        for j in range(3):
            digits = jnp.where(lane == j * rows + k, rest % DIGIT, digits)
            rest = rest // DIGIT
    line = jnp.concatenate([hidden_ref[...].astype(F32), digits.astype(F32)])
    out_ref[...] = jnp.broadcast_to(line[None], out_ref.shape).astype(BF16)


def spread(hidden, targets, chips):
    rows, width = hidden.shape
    return pl.pallas_call(
        spread_kernel,
        name="spread",
        out_shape=jax.ShapeDtypeStruct((chips, rows + 1, width), BF16),
        in_specs=[pl.BlockSpec(memory_space=pltpu.HBM)] * 2,
        out_specs=pl.BlockSpec(memory_space=pltpu.VMEM),
        scratch_shapes=[
            pltpu.SMEM(targets.shape, jnp.int32),
            pltpu.VMEM(hidden.shape, BF16),
            pltpu.SemaphoreType.DMA((2,)),
        ],
        compiler_params=pltpu.CompilerParams(vmem_limit_bytes=4 * MIB),
    )(in_hbm(targets), in_hbm(hidden))


def in_hbm(x):
    return pltpu.with_memory_space_constraint(x, pltpu.HBM)


def in_vmem(count):
    return [pl.BlockSpec(memory_space=pltpu.VMEM) for _ in range(count)]


def weights_for(lengths, rows):
    groups, seq_count = lengths.shape
    cores, x, yh, grps, z = (lax.axis_size(axis) for axis in ("core", "x", "yh", "grp", "z"))
    half, k, at_x, at_yh, at_grp, at_z = jnp.unravel_index(
        jnp.arange(cores * rows * x * yh * grps * z), (cores, rows, x, yh, grps, z)
    )
    core = (half + lax.axis_index("core")) % cores
    place = (((at_x * yh + at_yh) * z + at_z) * cores + core) * rows + k
    group_rows = place.shape[0] // groups
    before = jnp.arange(seq_count)[:, None] < jnp.arange(seq_count)[None, :]
    starts = jnp.sum(jnp.where(before[None], lengths[:, :, None], 0), axis=1)
    inside = (
        (at_grp[:, None, None] == jnp.arange(groups)[None, :, None])
        & (place[:, None, None] >= starts[None])
        & (place[:, None, None] < (starts + lengths)[None])
    )
    row_length = jnp.sum(jnp.where(inside, lengths[None].astype(F32), F32(0.0)), axis=(1, 2))
    return (group_rows / seq_count / row_length).reshape(1, -1)


def column(line):
    return jnp.broadcast_to(line, (128, line.shape[1])).T[:, :1]


def three_parts(x):
    high = x.astype(BF16).astype(F32)
    rest = x - high
    middle = rest.astype(BF16).astype(F32)
    return [high, middle, rest - middle]


def share_kernel(
    far, first_ref, given_ref, items_ref, log_ref, place_ref, states_ref, grad_ref, *rest
):
    scores, places, grad, picked = rest[-4:]
    rows = given_ref.shape[0] - 1
    chips = given_ref.shape[1]
    count, width = states_ref.shape
    items = items_ref.shape[0]
    block = min(BLOCK, items)
    lanes = min(128, block)
    digits = given_ref[rows].astype(F32)
    across = digits.T
    for k in range(rows):
        at = k * chips
        states_ref[at : at + chips, :] = given_ref[k]
        found = [digits[:, j * rows + k : j * rows + k + 1].astype(jnp.int32) for j in range(3)]
        found = found[0] + DIGIT * found[1] + DIGIT**2 * found[2] - first_ref[0]
        places[at : at + chips, :] = jnp.broadcast_to(found, (chips, lanes))
        found = [across[j * rows + k : j * rows + k + 1, :].astype(jnp.int32) for j in range(3)]
        found = found[0] + DIGIT * found[1] + DIGIT**2 * found[2] - first_ref[0]
        place_ref[:, at : at + chips] = found
    states = states_ref[...]
    high = None
    for at in range(0, items, block):
        found = lax.dot_general(
            states, items_ref[at : at + block, :], (((1,), (1,)), ((), ())), preferred_element_type=F32
        )
        scores[:, at : at + block] = found
        for c in range(0, block, lanes):
            top = found[:, c : c + lanes]
            high = top if high is None else jnp.maximum(high, top)
    high = jnp.max(high, axis=1, keepdims=True)
    total = None
    lane = lax.broadcasted_iota(jnp.int32, (1, lanes), 1)
    for at in range(0, items, block):
        others, hot = [], []
        for c in range(at, at + block, lanes):
            parts = jnp.exp(scores[:, c : c + lanes] - high)
            total = parts if total is None else total + parts
            matched = places[...] == lane + c
            others.append(jnp.where(matched, 0.0, parts).astype(BF16))
            hot.append(jnp.where(matched, 1.0, 0.0).astype(BF16))
        table = items_ref[at : at + block, :]
        more = jnp.dot(jnp.concatenate(others, axis=1), table, preferred_element_type=F32)
        grad[...] = more if at == 0 else grad[...] + more
        more = jnp.dot(jnp.concatenate(hot, axis=1), table, preferred_element_type=F32)
        picked[...] = more if at == 0 else picked[...] + more
    log_sum = high + jnp.log(jnp.sum(total, axis=1, keepdims=True))
    line = jnp.broadcast_to(log_sum, (count, 128)).T[:1, :]
    log_ref[...] = line
    share = grad[...] * jnp.exp(high - log_sum)
    if not far:
        grad_ref[...] = share
        rest[0][...] = picked[...].astype(BF16)
        return
    grad_ref[:count, :] = share.astype(BF16)
    grad_ref[count : 2 * count, :] = picked[...].astype(BF16)
    lines = [
        piece[:, at : at + chips] for piece in three_parts(line) for at in range(0, count, chips)
    ]
    lines = jnp.concatenate(lines + [jnp.zeros((-len(lines) % 16, chips), F32)])
    lines = jnp.concatenate([lines, jnp.zeros((lines.shape[0], width - chips), F32)], axis=1)
    grad_ref[2 * count :, :] = lines.astype(BF16)


def shares(far, first, given, items):
    height, chips, width = given.shape
    count = (height - 1) * chips
    lines = 3 * (height - 1)
    results = [
        jax.ShapeDtypeStruct((1, count), F32),
        jax.ShapeDtypeStruct((1, count), jnp.int32),
        jax.ShapeDtypeStruct((count, width), BF16),
    ]
    if far:
        results += [jax.ShapeDtypeStruct((2 * count + lines + -lines % 16, width), BF16)]
    else:
        results += [
            jax.ShapeDtypeStruct((count, width), F32),
            jax.ShapeDtypeStruct((count, width), BF16),
        ]
    return pl.pallas_call(
        lambda *refs: share_kernel(far, *refs),
        name="shares",
        out_shape=results,
        in_specs=[pl.BlockSpec(memory_space=pltpu.SMEM), *in_vmem(2)],
        out_specs=in_vmem(len(results)),
        scratch_shapes=[
            pltpu.VMEM((count, items.shape[0]), F32),
            pltpu.VMEM((count, min(128, BLOCK)), jnp.int32),
            pltpu.VMEM((count, width), F32),
            pltpu.VMEM((count, width), F32),
        ],
        compiler_params=pltpu.CompilerParams(vmem_limit_bytes=24 * MIB),
    )(first, given, items)


def pack_kernel(
    rows, own_grad_ref, own_rows_ref, other_ref, own_log_ref, far_log_ref, other_log_ref, out_ref
):
    length, _, width = out_ref.shape
    part = own_grad_ref.shape[0]
    own = jnp.concatenate([own_log_ref[...], far_log_ref[...]], axis=1)
    lines = other_ref[2 * part :, :].astype(F32)
    chips = part // rows
    other = [
        sum(lines[j * rows + k : j * rows + k + 1, :chips] for j in range(3)) for k in range(rows)
    ]
    other = jnp.concatenate(other + [other_log_ref[...]], axis=1)
    top = jnp.maximum(own, other)
    both = top + jnp.log(jnp.exp(own - top) + jnp.exp(other - top))
    grad = own_grad_ref[...] * column(jnp.exp(own - both)[:, :part])
    grad += other_ref[:part, :].astype(F32) * column(jnp.exp(other - both)[:, :part])
    picked = own_rows_ref[...].astype(F32) + other_ref[part : 2 * part, :].astype(F32)
    lines = [
        piece[:, at : at + width] for piece in three_parts(both) for at in range(0, 2 * part, width)
    ]
    lines = jnp.concatenate(lines)
    across = lambda x: [
        x.reshape(rows, length, -1, width)[k] for k in range(rows)
    ]
    sent = across(grad) + across(picked) + [jnp.broadcast_to(lines[None], (length, *lines.shape))]
    out_ref[...] = jnp.concatenate(sent, axis=1).astype(BF16)


def packed(rows, length, *pieces):
    part, width = pieces[0].shape
    lines = 3 * 2 * part // width
    height = 2 * (part // length) + lines
    return pl.pallas_call(
        lambda *refs: pack_kernel(rows, *refs),
        name="packed",
        out_shape=jax.ShapeDtypeStruct((length, height, width), BF16),
        in_specs=in_vmem(6),
        out_specs=pl.BlockSpec(memory_space=pltpu.VMEM),
        compiler_params=pltpu.CompilerParams(vmem_limit_bytes=12 * MIB),
    )(*pieces)


def merged(arrived_ref, at, wide):
    lines = arrived_ref[...].astype(F32)
    parts = sum(lines[:, at + j * wide : at + (j + 1) * wide] for j in range(3))
    top = jnp.max(parts, axis=0)
    logs = top + jnp.log(jnp.sum(jnp.exp(parts - top[None]), axis=0))
    return lines, jnp.exp(parts - logs[None]), logs


def middle_kernel(rows, plane_ref, arrived_ref, out_ref, turned, built):
    length = arrived_ref.shape[0]
    depth, height, width = out_ref.shape
    chips = length * depth
    wide = 2 * rows * chips // width
    kept = rows * depth
    lines, scale, logs = merged(arrived_ref, 2 * kept, wide)
    scale = scale.reshape(length * wide, width)
    pad = jnp.zeros((-(length * wide) % 128, width), F32)
    turned[...] = jnp.concatenate([scale, pad]).T
    for k in range(rows):
        c, lane = k * chips // width, k * chips % width
        across = turned[pl.ds(pl.multiple_of(plane_ref[0] * depth + lane, depth), depth), :]
        grad = jnp.zeros((depth, width), F32)
        picked = jnp.zeros((depth, width), F32)
        for j in range(length):
            at = j * wide + c
            grad += lines[j, k * depth : (k + 1) * depth] * across[:, at : at + 1]
            picked += lines[j, kept + k * depth : kept + (k + 1) * depth]
        for z in range(depth):
            built[z, k : k + 1, :] = grad[z : z + 1]
            built[z, rows + k : rows + k + 1, :] = picked[z : z + 1]
    lines = jnp.concatenate(three_parts(logs))
    at = 2 * rows
    built[:, at : at + 3 * wide, :] = jnp.broadcast_to(lines[None], (depth, 3 * wide, width))
    at += 3 * wide
    if height > at:
        built[:, at:, :] = jnp.zeros((depth, height - at, width), F32)
    out_ref[...] = built[...].astype(BF16)


def middle(rows, depth, plane, arrived):
    length, _, width = arrived.shape
    wide = 2 * rows * length * depth // width
    height = 2 * rows + 3 * wide
    height += -height % 8
    return pl.pallas_call(
        lambda *refs: middle_kernel(rows, *refs),
        name="middle",
        out_shape=jax.ShapeDtypeStruct((depth, height, width), BF16),
        in_specs=[pl.BlockSpec(memory_space=pltpu.SMEM), *in_vmem(1)],
        out_specs=pl.BlockSpec(memory_space=pltpu.VMEM),
        scratch_shapes=[
            pltpu.VMEM((width, length * wide + -(length * wide) % 128), F32),
            pltpu.VMEM((depth, height, width), F32),
        ],
        compiler_params=pltpu.CompilerParams(vmem_limit_bytes=12 * MIB),
    )(plane, arrived)


def last_kernel(
    chip_ref, arrived_ref, place_ref, far_place_ref, weight_ref, hidden_ref, states_ref,
    far_states_ref, items_ref, loss_hbm, hidden_grad_hbm, table_grad_hbm,
    states, buffer, loss_ref, hidden_grad_ref, sems,
):
    rows, width = hidden_ref.shape
    depth = arrived_ref.shape[0]
    items = items_ref.shape[0]
    count = states.shape[0]
    block = min(BLOCK, items)
    chips = count // (2 * rows)
    wide = count // width
    copies = []

    def send(source, target):
        copies.append(pltpu.make_async_copy(source, target, sems.at[len(copies)]))
        copies[-1].start()

    lines, scale, logs = merged(arrived_ref, 2 * rows, wide)
    weight = weight_ref[...]
    lane = lax.broadcasted_iota(jnp.int32, (1, width), 1)
    hidden = hidden_ref[...].astype(F32)
    place = lax.broadcasted_iota(jnp.int32, loss_ref.shape, 1)
    losses = jnp.zeros(loss_ref.shape, F32)
    grads = []
    for k in range(rows):
        c, first = k * chips // width, k * chips % width
        mine = lambda x: jnp.sum(
            jnp.where(lane == chip_ref[0] + first, x, 0.0), axis=-1, keepdims=True
        )
        log_total = mine(logs[c : c + 1])
        own_weight = mine(weight[:, c * width : (c + 1) * width])
        grad = jnp.zeros((1, width), F32)
        picked = jnp.zeros((1, width), F32)
        for j in range(depth):
            grad += lines[j, k : k + 1] * mine(scale[j, c : c + 1])
            picked += lines[j, rows + k : rows + k + 1]
        score = jnp.sum(hidden[k : k + 1] * picked, axis=1, keepdims=True)
        losses = jnp.where(place == k, log_total - score, losses)
        pull = (own_weight * (jnp.exp(score - log_total) - 1.0)).astype(BF16).astype(F32)
        grads.append(own_weight * grad + pull * picked)
    loss_ref[...] = losses
    send(loss_ref, loss_hbm)
    hidden_grad_ref[...] = jnp.concatenate(grads).astype(BF16)
    send(hidden_grad_ref, hidden_grad_hbm)
    line = jnp.concatenate([logs[c : c + 1] for c in range(wide)], axis=1)
    places = jnp.concatenate([place_ref[...], far_place_ref[...]], axis=1)
    states[: count // 2, :] = states_ref[...]
    states[count // 2 :, :] = far_states_ref[...]
    for at in range(0, items, block):
        scores = lax.dot_general(
            items_ref[at : at + block, :], states[...], (((1,), (1,)), ((), ())),
            preferred_element_type=F32,
        )
        parts = jnp.exp(scores - line)
        matched = lax.broadcasted_iota(jnp.int32, parts.shape, 0) == places - at
        signal = (weight * jnp.where(matched, parts - 1.0, parts)).astype(BF16)
        buffer[at : at + block, :] = jnp.dot(
            signal, states[...], preferred_element_type=F32
        ).astype(BF16)
        send(buffer.at[pl.ds(at, block)], table_grad_hbm.at[pl.ds(at, block)])
    for copy in copies:
        copy.wait()


def last(chip, arrived, place, far_place, weight, hidden, states, far_states, items):
    rows, width = hidden.shape
    return pl.pallas_call(
        last_kernel,
        name="last",
        out_shape=(
            jax.ShapeDtypeStruct((1, rows), F32),
            jax.ShapeDtypeStruct((rows, width), BF16),
            jax.ShapeDtypeStruct(items.shape, BF16),
        ),
        in_specs=[pl.BlockSpec(memory_space=pltpu.SMEM), *in_vmem(8)],
        out_specs=[pl.BlockSpec(memory_space=pltpu.HBM)] * 3,
        scratch_shapes=[
            pltpu.VMEM((2 * states.shape[0], width), BF16),
            pltpu.VMEM(items.shape, BF16),
            pltpu.VMEM((1, rows), F32),
            pltpu.VMEM((rows, width), BF16),
            pltpu.SemaphoreType.DMA((2 + items.shape[0] // min(BLOCK, items.shape[0]),)),
        ],
        compiler_params=pltpu.CompilerParams(vmem_limit_bytes=16 * MIB),
    )(chip, arrived, place, far_place, weight, hidden, states, far_states, items)


def steps(hidden, item_table, targets, lengths):
    rows, _ = hidden.shape
    group = lax.axis_index("grp")
    chip = lax.axis_index(CHIPS).reshape(1)
    own_items = item_table.shape[0] // 2
    items = lax.dynamic_slice_in_dim(item_table, group * own_items, own_items)
    first_own = (lax.axis_index(ITEM) * 2 + group) * own_items
    weight = weights_for(lengths, rows)
    sent = spread(hidden, targets, lax.axis_size(CHIPS))
    mine = lax.all_to_all(sent, CHIPS, 0, 0, tiled=True)
    mine = jnp.swapaxes(mine, 0, 1)
    first_own = first_own.reshape(1)
    other = from_pair(mine)
    own_logs, place, states, own_grad, own_picked = shares(False, first_own, mine, items)
    other_logs = from_pair(own_logs)
    far_logs, far_place, far_states, far_share = shares(True, first_own, other, items)
    sent = packed(
        rows, lax.axis_size(PLANE), own_grad, own_picked, from_pair(far_share),
        own_logs, far_logs, other_logs,
    )
    arrived = lax.all_to_all(sent, PLANE, 0, 0, tiled=True)
    sent = middle(rows, lax.axis_size("z"), lax.axis_index(PLANE).reshape(1), arrived)
    arrived = lax.all_to_all(sent, "z", 0, 0, tiled=True)
    row_loss, hidden_grad, table_grad = last(
        chip, arrived, place, far_place, weight, hidden, states, far_states, items
    )
    return (row_loss.reshape(-1), hidden_grad, table_grad)


def mapped(split):
    return jax.shard_map(
        steps,
        mesh=split,
        in_specs=(P(GRP_ITEM, None), P(ITEM, None), P(GRP_ITEM), P()),
        out_specs=(P(GRP_ITEM), P(GRP_ITEM, None), P(ITEM_GRP, None)),
        check_vma=False,
    )


def solution(mesh):
    split = Mesh(
        mesh.devices.reshape(4, 2, 8, 2, mesh.shape["grp"]),
        ("x", "yh", "z", "core", "grp"),
    )
    return mapped(split)
```

```python
import jax
import jax.numpy as jnp
from jax import lax
from jax.experimental import pallas as pl
from jax.experimental.pallas import tpu as pltpu
from jax.sharding import Mesh
from jax.sharding import PartitionSpec as P

ITEM = ("x", "yh", "z", "core")
GRP_ITEM = ("grp", "x", "yh", "z", "core")
ITEM_GRP = ("x", "yh", "z", "core", "grp")
PLANE = ("x", "yh", "grp")
CHIPS = ("x", "yh", "grp", "z")
DIGIT = 128
BLOCK = 512
MIB = 1 << 20
F32 = jnp.float32
BF16 = jnp.bfloat16


def from_pair(x):
    return lax.ppermute(x, "core", [(0, 1), (1, 0)])


def spread_kernel(targets_hbm, hidden_hbm, out_ref, targets_ref, hidden_ref, sems):
    copies = [
        pltpu.make_async_copy(targets_hbm, targets_ref, sems.at[0]),
        pltpu.make_async_copy(hidden_hbm, hidden_ref, sems.at[1]),
    ]
    for copy in copies:
        copy.start()
    for copy in copies:
        copy.wait()
    _, height, width = out_ref.shape
    rows = height - 1
    lane = lax.broadcasted_iota(jnp.int32, (1, width), 1)
    digits = jnp.zeros((1, width), jnp.int32)
    for k in range(rows):
        rest = targets_ref[k]
        for j in range(3):
            digits = jnp.where(lane == j * rows + k, rest % DIGIT, digits)
            rest = rest // DIGIT
    line = jnp.concatenate([hidden_ref[...].astype(F32), digits.astype(F32)])
    out_ref[...] = jnp.broadcast_to(line[None], out_ref.shape).astype(BF16)


def spread(hidden, targets, chips):
    rows, width = hidden.shape
    return pl.pallas_call(
        spread_kernel,
        name="spread",
        out_shape=jax.ShapeDtypeStruct((chips, rows + 1, width), BF16),
        in_specs=[pl.BlockSpec(memory_space=pltpu.HBM)] * 2,
        out_specs=pl.BlockSpec(memory_space=pltpu.VMEM),
        scratch_shapes=[
            pltpu.SMEM(targets.shape, jnp.int32),
            pltpu.VMEM(hidden.shape, BF16),
            pltpu.SemaphoreType.DMA((2,)),
        ],
        compiler_params=pltpu.CompilerParams(vmem_limit_bytes=4 * MIB),
    )(in_hbm(targets), in_hbm(hidden))


def in_hbm(x):
    return pltpu.with_memory_space_constraint(x, pltpu.HBM)


def in_vmem(count):
    return [pl.BlockSpec(memory_space=pltpu.VMEM) for _ in range(count)]


def weights_for(lengths, rows):
    groups, seq_count = lengths.shape
    cores, x, yh, grps, z = (lax.axis_size(axis) for axis in ("core", "x", "yh", "grp", "z"))
    half, k, at_x, at_yh, at_grp, at_z = jnp.unravel_index(
        jnp.arange(cores * rows * x * yh * grps * z), (cores, rows, x, yh, grps, z)
    )
    core = (half + lax.axis_index("core")) % cores
    place = (((at_x * yh + at_yh) * z + at_z) * cores + core) * rows + k
    group_rows = place.shape[0] // groups
    before = jnp.arange(seq_count)[:, None] < jnp.arange(seq_count)[None, :]
    starts = jnp.sum(jnp.where(before[None], lengths[:, :, None], 0), axis=1)
    inside = (
        (at_grp[:, None, None] == jnp.arange(groups)[None, :, None])
        & (place[:, None, None] >= starts[None])
        & (place[:, None, None] < (starts + lengths)[None])
    )
    row_length = jnp.sum(jnp.where(inside, lengths[None].astype(F32), F32(0.0)), axis=(1, 2))
    return (group_rows / seq_count / row_length).reshape(1, -1)


def column(line):
    return jnp.broadcast_to(line, (128, line.shape[1])).T[:, :1]


def three_parts(x):
    high = x.astype(BF16).astype(F32)
    rest = x - high
    middle = rest.astype(BF16).astype(F32)
    return [high, middle, rest - middle]


def share_kernel(
    far, first_ref, given_ref, items_ref, near_log_ref, log_ref, place_ref, states_ref, grad_ref,
    *rest,
):
    scores, places, grad, picked = rest[-4:]
    rows = given_ref.shape[0] - 1
    chips = given_ref.shape[1]
    count, width = states_ref.shape
    items = items_ref.shape[0]
    block = min(BLOCK, items)
    lanes = min(128, block)
    digits = given_ref[rows].astype(F32)
    across = digits.T
    for k in range(rows):
        at = k * chips
        states_ref[at : at + chips, :] = given_ref[k]
        found = [digits[:, j * rows + k : j * rows + k + 1].astype(jnp.int32) for j in range(3)]
        found = found[0] + DIGIT * found[1] + DIGIT**2 * found[2] - first_ref[0]
        places[at : at + chips, :] = jnp.broadcast_to(found, (chips, lanes))
        found = [across[j * rows + k : j * rows + k + 1, :].astype(jnp.int32) for j in range(3)]
        found = found[0] + DIGIT * found[1] + DIGIT**2 * found[2] - first_ref[0]
        place_ref[:, at : at + chips] = found
    states = states_ref[...]
    high = None
    for at in range(0, items, block):
        found = lax.dot_general(
            states, items_ref[at : at + block, :], (((1,), (1,)), ((), ())), preferred_element_type=F32
        )
        scores[:, at : at + block] = found
        for c in range(0, block, lanes):
            top = found[:, c : c + lanes]
            high = top if high is None else jnp.maximum(high, top)
    high = jnp.max(high, axis=1, keepdims=True)
    total = None
    lane = lax.broadcasted_iota(jnp.int32, (1, lanes), 1)
    for at in range(0, items, block):
        others, hot = [], []
        for c in range(at, at + block, lanes):
            parts = jnp.exp(scores[:, c : c + lanes] - high)
            total = parts if total is None else total + parts
            matched = places[...] == lane + c
            others.append(jnp.where(matched, 0.0, parts).astype(BF16))
            hot.append(jnp.where(matched, 1.0, 0.0).astype(BF16))
        table = items_ref[at : at + block, :]
        more = jnp.dot(jnp.concatenate(others, axis=1), table, preferred_element_type=F32)
        grad[...] = more if at == 0 else grad[...] + more
        more = jnp.dot(jnp.concatenate(hot, axis=1), table, preferred_element_type=F32)
        picked[...] = more if at == 0 else picked[...] + more
    log_sum = high + jnp.log(jnp.sum(total, axis=1, keepdims=True))
    line = jnp.broadcast_to(log_sum, (count, 128)).T[:1, :]
    log_ref[...] = line
    share = grad[...] * jnp.exp(high - log_sum)
    if not far:
        grad_ref[...] = share
        rest[0][...] = picked[...].astype(BF16)
        return
    grad_ref[:count, :] = share.astype(BF16)
    grad_ref[count : 2 * count, :] = picked[...].astype(BF16)
    lines = [
        piece[:, at : at + chips]
        for source in (line, near_log_ref[...])
        for piece in three_parts(source)
        for at in range(0, count, chips)
    ]
    lines = jnp.concatenate(lines + [jnp.zeros((-len(lines) % 16, chips), F32)])
    lines = jnp.concatenate([lines, jnp.zeros((lines.shape[0], width - chips), F32)], axis=1)
    grad_ref[2 * count :, :] = lines.astype(BF16)


def shares(far, first, given, items, near_logs):
    height, chips, width = given.shape
    count = (height - 1) * chips
    lines = 6 * (height - 1)
    results = [
        jax.ShapeDtypeStruct((1, count), F32),
        jax.ShapeDtypeStruct((1, count), jnp.int32),
        jax.ShapeDtypeStruct((count, width), BF16),
    ]
    if far:
        results += [jax.ShapeDtypeStruct((2 * count + lines + -lines % 16, width), BF16)]
    else:
        results += [
            jax.ShapeDtypeStruct((count, width), F32),
            jax.ShapeDtypeStruct((count, width), BF16),
        ]
    return pl.pallas_call(
        lambda *refs: share_kernel(far, *refs),
        name="shares",
        out_shape=results,
        in_specs=[pl.BlockSpec(memory_space=pltpu.SMEM), *in_vmem(3)],
        out_specs=in_vmem(len(results)),
        scratch_shapes=[
            pltpu.VMEM((count, items.shape[0]), F32),
            pltpu.VMEM((count, min(128, BLOCK)), jnp.int32),
            pltpu.VMEM((count, width), F32),
            pltpu.VMEM((count, width), F32),
        ],
        compiler_params=pltpu.CompilerParams(vmem_limit_bytes=24 * MIB),
    )(first, given, items, near_logs)


def pack_kernel(
    rows, own_grad_ref, own_rows_ref, other_ref, own_log_ref, far_log_ref, out_ref
):
    length, _, width = out_ref.shape
    part = own_grad_ref.shape[0]
    own = jnp.concatenate([own_log_ref[...], far_log_ref[...]], axis=1)
    lines = other_ref[2 * part :, :].astype(F32)
    chips = part // rows
    other = [
        sum(lines[at + j * rows + k : at + j * rows + k + 1, :chips] for j in range(3))
        for at in (0, 3 * rows)
        for k in range(rows)
    ]
    other = jnp.concatenate(other, axis=1)
    top = jnp.maximum(own, other)
    both = top + jnp.log(jnp.exp(own - top) + jnp.exp(other - top))
    grad = own_grad_ref[...] * column(jnp.exp(own - both)[:, :part])
    grad += other_ref[:part, :].astype(F32) * column(jnp.exp(other - both)[:, :part])
    picked = own_rows_ref[...].astype(F32) + other_ref[part : 2 * part, :].astype(F32)
    lines = [
        piece[:, at : at + width] for piece in three_parts(both) for at in range(0, 2 * part, width)
    ]
    lines = jnp.concatenate(lines)
    across = lambda x: [
        x.reshape(rows, length, -1, width)[k] for k in range(rows)
    ]
    sent = across(grad) + across(picked) + [jnp.broadcast_to(lines[None], (length, *lines.shape))]
    out_ref[...] = jnp.concatenate(sent, axis=1).astype(BF16)


def packed(rows, length, *pieces):
    part, width = pieces[0].shape
    lines = 3 * 2 * part // width
    height = 2 * (part // length) + lines
    return pl.pallas_call(
        lambda *refs: pack_kernel(rows, *refs),
        name="packed",
        out_shape=jax.ShapeDtypeStruct((length, height, width), BF16),
        in_specs=in_vmem(5),
        out_specs=pl.BlockSpec(memory_space=pltpu.VMEM),
        compiler_params=pltpu.CompilerParams(vmem_limit_bytes=12 * MIB),
    )(*pieces)


def merged(arrived_ref, at, wide):
    lines = arrived_ref[...].astype(F32)
    parts = sum(lines[:, at + j * wide : at + (j + 1) * wide] for j in range(3))
    top = jnp.max(parts, axis=0)
    logs = top + jnp.log(jnp.sum(jnp.exp(parts - top[None]), axis=0))
    return lines, jnp.exp(parts - logs[None]), logs


def middle_kernel(rows, plane_ref, arrived_ref, out_ref, turned, built):
    length = arrived_ref.shape[0]
    depth, height, width = out_ref.shape
    chips = length * depth
    wide = 2 * rows * chips // width
    kept = rows * depth
    lines, scale, logs = merged(arrived_ref, 2 * kept, wide)
    scale = scale.reshape(length * wide, width)
    pad = jnp.zeros((-(length * wide) % 128, width), F32)
    turned[...] = jnp.concatenate([scale, pad]).T
    for k in range(rows):
        c, lane = k * chips // width, k * chips % width
        across = turned[pl.ds(pl.multiple_of(plane_ref[0] * depth + lane, depth), depth), :]
        grad = jnp.zeros((depth, width), F32)
        picked = jnp.zeros((depth, width), F32)
        for j in range(length):
            at = j * wide + c
            grad += lines[j, k * depth : (k + 1) * depth] * across[:, at : at + 1]
            picked += lines[j, kept + k * depth : kept + (k + 1) * depth]
        for z in range(depth):
            built[z, k : k + 1, :] = grad[z : z + 1]
            built[z, rows + k : rows + k + 1, :] = picked[z : z + 1]
    lines = jnp.concatenate(three_parts(logs))
    at = 2 * rows
    built[:, at : at + 3 * wide, :] = jnp.broadcast_to(lines[None], (depth, 3 * wide, width))
    at += 3 * wide
    if height > at:
        built[:, at:, :] = jnp.zeros((depth, height - at, width), F32)
    out_ref[...] = built[...].astype(BF16)


def middle(rows, depth, plane, arrived):
    length, _, width = arrived.shape
    wide = 2 * rows * length * depth // width
    height = 2 * rows + 3 * wide
    height += -height % 8
    return pl.pallas_call(
        lambda *refs: middle_kernel(rows, *refs),
        name="middle",
        out_shape=jax.ShapeDtypeStruct((depth, height, width), BF16),
        in_specs=[pl.BlockSpec(memory_space=pltpu.SMEM), *in_vmem(1)],
        out_specs=pl.BlockSpec(memory_space=pltpu.VMEM),
        scratch_shapes=[
            pltpu.VMEM((width, length * wide + -(length * wide) % 128), F32),
            pltpu.VMEM((depth, height, width), F32),
        ],
        compiler_params=pltpu.CompilerParams(vmem_limit_bytes=12 * MIB),
    )(plane, arrived)


def early_kernel(log_ref, far_log_ref, states_ref, far_states_ref, items_ref, out_ref, states):
    part = states_ref.shape[0]
    items, block = out_ref.shape[0], min(BLOCK, items_ref.shape[0])
    first = items_ref.shape[0] - items
    states[:part, :] = states_ref[...]
    states[part:, :] = far_states_ref[...]
    logs = jnp.concatenate([log_ref[...], far_log_ref[...]], axis=1)
    for at in range(0, items, block):
        scores = lax.dot_general(
            items_ref[first + at : first + at + block, :], states[...], (((1,), (1,)), ((), ())),
            preferred_element_type=F32,
        )
        out_ref[at : at + block, :] = jnp.exp(scores - logs)


def early(logs, far_logs, states, far_states, items):
    part, width = states.shape
    block = min(BLOCK, items.shape[0])
    steps = items.shape[0] // block // 2
    return pl.pallas_call(
        early_kernel,
        name="early",
        out_shape=jax.ShapeDtypeStruct((steps * block, 2 * part), F32),
        in_specs=in_vmem(5),
        out_specs=pl.BlockSpec(memory_space=pltpu.VMEM),
        scratch_shapes=[pltpu.VMEM((2 * part, width), BF16)],
        compiler_params=pltpu.CompilerParams(vmem_limit_bytes=24 * MIB),
    )(logs, far_logs, states, far_states, items)


def last_kernel(
    chip_ref, arrived_ref, place_ref, far_place_ref, weight_ref, hidden_ref, states_ref,
    far_states_ref, items_ref, log_ref, far_log_ref, early_hbm,
    loss_hbm, hidden_grad_hbm, table_grad_hbm,
    states, buffer, loss_ref, hidden_grad_ref, early_ref, sems, early_sems,
):
    rows, width = hidden_ref.shape
    depth = arrived_ref.shape[0]
    items = items_ref.shape[0]
    count = states.shape[0]
    block = min(BLOCK, items)
    chips = count // (2 * rows)
    wide = count // width
    copies = []
    fetches = [
        pltpu.make_async_copy(
            early_hbm.at[pl.ds(at, block)], early_ref.at[pl.ds(at, block)], early_sems.at[step]
        )
        for step, at in enumerate(range(0, early_ref.shape[0], block))
    ]
    for fetch in fetches:
        fetch.start()

    def send(source, target):
        copies.append(pltpu.make_async_copy(source, target, sems.at[len(copies)]))
        copies[-1].start()

    lines, scale, logs = merged(arrived_ref, 2 * rows, wide)
    weight = weight_ref[...]
    lane = lax.broadcasted_iota(jnp.int32, (1, width), 1)
    hidden = hidden_ref[...].astype(F32)
    place = lax.broadcasted_iota(jnp.int32, loss_ref.shape, 1)
    losses = jnp.zeros(loss_ref.shape, F32)
    grads = []
    for k in range(rows):
        c, first = k * chips // width, k * chips % width
        mine = lambda x: jnp.sum(
            jnp.where(lane == chip_ref[0] + first, x, 0.0), axis=-1, keepdims=True
        )
        log_total = mine(logs[c : c + 1])
        own_weight = mine(weight[:, c * width : (c + 1) * width])
        grad = jnp.zeros((1, width), F32)
        picked = jnp.zeros((1, width), F32)
        for j in range(depth):
            grad += lines[j, k : k + 1] * mine(scale[j, c : c + 1])
            picked += lines[j, rows + k : rows + k + 1]
        score = jnp.sum(hidden[k : k + 1] * picked, axis=1, keepdims=True)
        losses = jnp.where(place == k, log_total - score, losses)
        pull = (own_weight * (jnp.exp(score - log_total) - 1.0)).astype(BF16).astype(F32)
        grads.append(own_weight * grad + pull * picked)
    loss_ref[...] = losses
    send(loss_ref, loss_hbm)
    hidden_grad_ref[...] = jnp.concatenate(grads).astype(BF16)
    send(hidden_grad_ref, hidden_grad_hbm)
    line = jnp.concatenate([logs[c : c + 1] for c in range(wide)], axis=1)
    places = jnp.concatenate([place_ref[...], far_place_ref[...]], axis=1)
    states[: count // 2, :] = states_ref[...]
    states[count // 2 :, :] = far_states_ref[...]
    given = jnp.concatenate([log_ref[...], far_log_ref[...]], axis=1)
    factor = weight * jnp.exp(given - line)
    first = items - early_ref.shape[0]
    for at in range(0, items, block):
        matched = lax.broadcasted_iota(jnp.int32, (block, count), 0) == places - at
        if at < first:
            scores = lax.dot_general(
                items_ref[at : at + block, :], states[...], (((1,), (1,)), ((), ())),
                preferred_element_type=F32,
            )
            parts = jnp.exp(scores - line)
            signal = (weight * jnp.where(matched, parts - 1.0, parts)).astype(BF16)
        else:
            fetches[(at - first) // block].wait()
            parts = early_ref[at - first : at - first + block, :] * factor
            signal = jnp.where(matched, parts - weight, parts).astype(BF16)
        buffer[at : at + block, :] = jnp.dot(
            signal, states[...], preferred_element_type=F32
        ).astype(BF16)
        send(buffer.at[pl.ds(at, block)], table_grad_hbm.at[pl.ds(at, block)])
    for copy in copies:
        copy.wait()


def last(
    chip, arrived, place, far_place, weight, hidden, states, far_states, items, logs, far_logs, parts
):
    rows, width = hidden.shape
    return pl.pallas_call(
        last_kernel,
        name="last",
        out_shape=(
            jax.ShapeDtypeStruct((1, rows), F32),
            jax.ShapeDtypeStruct((rows, width), BF16),
            jax.ShapeDtypeStruct(items.shape, BF16),
        ),
        in_specs=[pl.BlockSpec(memory_space=pltpu.SMEM), *in_vmem(10), pl.BlockSpec(memory_space=pltpu.HBM)],
        out_specs=[pl.BlockSpec(memory_space=pltpu.HBM)] * 3,
        scratch_shapes=[
            pltpu.VMEM((2 * states.shape[0], width), BF16),
            pltpu.VMEM(items.shape, BF16),
            pltpu.VMEM((1, rows), F32),
            pltpu.VMEM((rows, width), BF16),
            pltpu.VMEM(parts.shape, F32),
            pltpu.SemaphoreType.DMA((2 + items.shape[0] // min(BLOCK, items.shape[0]),)),
            pltpu.SemaphoreType.DMA((parts.shape[0] // min(BLOCK, items.shape[0]),)),
        ],
        compiler_params=pltpu.CompilerParams(vmem_limit_bytes=24 * MIB),
    )(
        chip, arrived, place, far_place, weight, hidden, states, far_states, items,
        logs, far_logs, in_hbm(parts),
    )


def steps(hidden, item_table, targets, lengths):
    rows, _ = hidden.shape
    group = lax.axis_index("grp")
    chip = lax.axis_index(CHIPS).reshape(1)
    own_items = item_table.shape[0] // 2
    items = lax.dynamic_slice_in_dim(item_table, group * own_items, own_items)
    first_own = (lax.axis_index(ITEM) * 2 + group) * own_items
    weight = weights_for(lengths, rows)
    sent = spread(hidden, targets, lax.axis_size(CHIPS))
    mine = lax.all_to_all(sent, CHIPS, 0, 0, tiled=True)
    mine = jnp.swapaxes(mine, 0, 1)
    first_own = first_own.reshape(1)
    other = from_pair(mine)
    no_logs = jnp.zeros((1, rows * lax.axis_size(CHIPS)), F32)
    own_logs, place, states, own_grad, own_picked = shares(False, first_own, mine, items, no_logs)
    far_logs, far_place, far_states, far_share = shares(
        True, first_own, other, items, own_logs
    )
    sent = packed(
        rows, lax.axis_size(PLANE), own_grad, own_picked, from_pair(far_share),
        own_logs, far_logs,
    )
    arrived = lax.all_to_all(sent, PLANE, 0, 0, tiled=True)
    sent = middle(rows, lax.axis_size("z"), lax.axis_index(PLANE).reshape(1), arrived)
    arrived = lax.all_to_all(sent, "z", 0, 0, tiled=True)
    parts = early(own_logs, far_logs, states, far_states, items)
    row_loss, hidden_grad, table_grad = last(
        chip, arrived, place, far_place, weight, hidden, states, far_states, items,
        own_logs, far_logs, parts,
    )
    return (row_loss.reshape(-1), hidden_grad, table_grad)


def mapped(split):
    return jax.shard_map(
        steps,
        mesh=split,
        in_specs=(P(GRP_ITEM, None), P(ITEM, None), P(GRP_ITEM), P()),
        out_specs=(P(GRP_ITEM), P(GRP_ITEM, None), P(ITEM_GRP, None)),
        check_vma=False,
    )


def solution(mesh):
    split = Mesh(
        mesh.devices.reshape(4, 2, 8, 2, mesh.shape["grp"]),
        ("x", "yh", "z", "core", "grp"),
    )
    return mapped(split)
```

```python
import jax
import jax.numpy as jnp
from jax import lax
from jax.experimental import pallas as pl
from jax.experimental.pallas import tpu as pltpu
from jax.sharding import Mesh
from jax.sharding import PartitionSpec as P

ITEM = ("x", "yh", "z", "core")
GRP_ITEM = ("grp", "x", "yh", "z", "core")
ITEM_GRP = ("x", "yh", "z", "core", "grp")
PLANE = ("x", "yh", "grp")
CHIPS = ("x", "yh", "grp", "z")
DIGIT = 128
BLOCK = 512
MIB = 1 << 20
F32 = jnp.float32
BF16 = jnp.bfloat16


def from_pair(x):
    return lax.ppermute(x, "core", [(0, 1), (1, 0)])


def spread_kernel(targets_hbm, hidden_hbm, out_ref, targets_ref, hidden_ref, sems):
    copies = [
        pltpu.make_async_copy(targets_hbm, targets_ref, sems.at[0]),
        pltpu.make_async_copy(hidden_hbm, hidden_ref, sems.at[1]),
    ]
    for copy in copies:
        copy.start()
    for copy in copies:
        copy.wait()
    _, height, width = out_ref.shape
    rows = height - 1
    lane = lax.broadcasted_iota(jnp.int32, (1, width), 1)
    digits = jnp.zeros((1, width), jnp.int32)
    for k in range(rows):
        rest = targets_ref[k]
        for j in range(3):
            digits = jnp.where(lane == j * rows + k, rest % DIGIT, digits)
            rest = rest // DIGIT
    line = jnp.concatenate([hidden_ref[...].astype(F32), digits.astype(F32)])
    out_ref[...] = jnp.broadcast_to(line[None], out_ref.shape).astype(BF16)


def spread(hidden, targets, chips):
    rows, width = hidden.shape
    return pl.pallas_call(
        spread_kernel,
        name="spread",
        out_shape=jax.ShapeDtypeStruct((chips, rows + 1, width), BF16),
        in_specs=[pl.BlockSpec(memory_space=pltpu.HBM)] * 2,
        out_specs=pl.BlockSpec(memory_space=pltpu.VMEM),
        scratch_shapes=[
            pltpu.SMEM(targets.shape, jnp.int32),
            pltpu.VMEM(hidden.shape, BF16),
            pltpu.SemaphoreType.DMA((2,)),
        ],
        compiler_params=pltpu.CompilerParams(vmem_limit_bytes=4 * MIB),
    )(in_hbm(targets), in_hbm(hidden))


def in_hbm(x):
    return pltpu.with_memory_space_constraint(x, pltpu.HBM)


def in_vmem(count):
    return [pl.BlockSpec(memory_space=pltpu.VMEM) for _ in range(count)]


def weights_for(lengths, rows):
    groups, seq_count = lengths.shape
    cores, x, yh, grps, z = (lax.axis_size(axis) for axis in ("core", "x", "yh", "grp", "z"))
    half, k, at_x, at_yh, at_grp, at_z = jnp.unravel_index(
        jnp.arange(cores * rows * x * yh * grps * z), (cores, rows, x, yh, grps, z)
    )
    core = (half + lax.axis_index("core")) % cores
    place = (((at_x * yh + at_yh) * z + at_z) * cores + core) * rows + k
    group_rows = place.shape[0] // groups
    before = jnp.arange(seq_count)[:, None] < jnp.arange(seq_count)[None, :]
    starts = jnp.sum(jnp.where(before[None], lengths[:, :, None], 0), axis=1)
    inside = (
        (at_grp[:, None, None] == jnp.arange(groups)[None, :, None])
        & (place[:, None, None] >= starts[None])
        & (place[:, None, None] < (starts + lengths)[None])
    )
    row_length = jnp.sum(jnp.where(inside, lengths[None].astype(F32), F32(0.0)), axis=(1, 2))
    return (group_rows / seq_count / row_length).reshape(1, -1)


def column(line):
    return jnp.broadcast_to(line, (128, line.shape[1])).T[:, :1]


def three_parts(x):
    high = x.astype(BF16).astype(F32)
    rest = x - high
    middle = rest.astype(BF16).astype(F32)
    return [high, middle, rest - middle]


def share_kernel(
    far, first_ref, given_ref, items_ref, near_log_ref, log_ref, place_ref, states_ref, grad_ref,
    *rest,
):
    scores, places, grad, picked = rest[-4:]
    rows = given_ref.shape[0] - 1
    chips = given_ref.shape[1]
    count, width = states_ref.shape
    items = items_ref.shape[0]
    block = min(BLOCK, items)
    lanes = min(128, block)
    digits = given_ref[rows].astype(F32)
    across = digits.T
    for k in range(rows):
        at = k * chips
        states_ref[at : at + chips, :] = given_ref[k]
        found = [digits[:, j * rows + k : j * rows + k + 1].astype(jnp.int32) for j in range(3)]
        found = found[0] + DIGIT * found[1] + DIGIT**2 * found[2] - first_ref[0]
        places[at : at + chips, :] = jnp.broadcast_to(found, (chips, lanes))
        found = [across[j * rows + k : j * rows + k + 1, :].astype(jnp.int32) for j in range(3)]
        found = found[0] + DIGIT * found[1] + DIGIT**2 * found[2] - first_ref[0]
        place_ref[:, at : at + chips] = found
    states = states_ref[...]
    high = None
    for at in range(0, items, block):
        found = lax.dot_general(
            states, items_ref[at : at + block, :], (((1,), (1,)), ((), ())), preferred_element_type=F32
        )
        scores[:, at : at + block] = found
        for c in range(0, block, lanes):
            top = found[:, c : c + lanes]
            high = top if high is None else jnp.maximum(high, top)
    high = jnp.max(high, axis=1, keepdims=True)
    total = None
    lane = lax.broadcasted_iota(jnp.int32, (1, lanes), 1)
    for at in range(0, items, block):
        others, hot = [], []
        for c in range(at, at + block, lanes):
            parts = jnp.exp(scores[:, c : c + lanes] - high)
            total = parts if total is None else total + parts
            matched = places[...] == lane + c
            others.append(jnp.where(matched, 0.0, parts).astype(BF16))
            hot.append(jnp.where(matched, 1.0, 0.0).astype(BF16))
        table = items_ref[at : at + block, :]
        more = jnp.dot(jnp.concatenate(others, axis=1), table, preferred_element_type=F32)
        grad[...] = more if at == 0 else grad[...] + more
        more = jnp.dot(jnp.concatenate(hot, axis=1), table, preferred_element_type=F32)
        picked[...] = more if at == 0 else picked[...] + more
    log_sum = high + jnp.log(jnp.sum(total, axis=1, keepdims=True))
    line = jnp.broadcast_to(log_sum, (count, 128)).T[:1, :]
    log_ref[...] = line
    share = grad[...] * jnp.exp(high - log_sum)
    if not far:
        grad_ref[...] = share
        rest[0][...] = picked[...].astype(BF16)
        return
    grad_ref[:count, :] = share.astype(BF16)
    grad_ref[count : 2 * count, :] = picked[...].astype(BF16)
    lines = [
        piece[:, at : at + chips]
        for source in (line, near_log_ref[...])
        for piece in three_parts(source)
        for at in range(0, count, chips)
    ]
    lines = jnp.concatenate(lines + [jnp.zeros((-len(lines) % 16, chips), F32)])
    lines = jnp.concatenate([lines, jnp.zeros((lines.shape[0], width - chips), F32)], axis=1)
    grad_ref[2 * count :, :] = lines.astype(BF16)


def shares(far, first, given, items, near_logs):
    height, chips, width = given.shape
    count = (height - 1) * chips
    lines = 6 * (height - 1)
    results = [
        jax.ShapeDtypeStruct((1, count), F32),
        jax.ShapeDtypeStruct((1, count), jnp.int32),
        jax.ShapeDtypeStruct((count, width), BF16),
    ]
    if far:
        results += [jax.ShapeDtypeStruct((2 * count + lines + -lines % 16, width), BF16)]
    else:
        results += [
            jax.ShapeDtypeStruct((count, width), F32),
            jax.ShapeDtypeStruct((count, width), BF16),
        ]
    return pl.pallas_call(
        lambda *refs: share_kernel(far, *refs),
        name="shares",
        out_shape=results,
        in_specs=[pl.BlockSpec(memory_space=pltpu.SMEM), *in_vmem(3)],
        out_specs=in_vmem(len(results)),
        scratch_shapes=[
            pltpu.VMEM((count, items.shape[0]), F32),
            pltpu.VMEM((count, min(128, BLOCK)), jnp.int32),
            pltpu.VMEM((count, width), F32),
            pltpu.VMEM((count, width), F32),
        ],
        compiler_params=pltpu.CompilerParams(vmem_limit_bytes=24 * MIB),
    )(first, given, items, near_logs)


def pack_kernel(
    rows, own_grad_ref, own_rows_ref, other_ref, own_log_ref, far_log_ref, out_ref
):
    length, _, width = out_ref.shape
    part = own_grad_ref.shape[0]
    own = jnp.concatenate([own_log_ref[...], far_log_ref[...]], axis=1)
    lines = other_ref[2 * part :, :].astype(F32)
    chips = part // rows
    other = [
        sum(lines[at + j * rows + k : at + j * rows + k + 1, :chips] for j in range(3))
        for at in (0, 3 * rows)
        for k in range(rows)
    ]
    other = jnp.concatenate(other, axis=1)
    top = jnp.maximum(own, other)
    both = top + jnp.log(jnp.exp(own - top) + jnp.exp(other - top))
    grad = own_grad_ref[...] * column(jnp.exp(own - both)[:, :part])
    grad += other_ref[:part, :].astype(F32) * column(jnp.exp(other - both)[:, :part])
    picked = own_rows_ref[...].astype(F32) + other_ref[part : 2 * part, :].astype(F32)
    lines = [
        piece[:, at : at + width] for piece in three_parts(both) for at in range(0, 2 * part, width)
    ]
    lines = jnp.concatenate(lines)
    across = lambda x: [
        x.reshape(rows, length, -1, width)[k] for k in range(rows)
    ]
    sent = across(grad) + across(picked) + [jnp.broadcast_to(lines[None], (length, *lines.shape))]
    out_ref[...] = jnp.concatenate(sent, axis=1).astype(BF16)


def packed(rows, length, *pieces):
    part, width = pieces[0].shape
    lines = 3 * 2 * part // width
    height = 2 * (part // length) + lines
    return pl.pallas_call(
        lambda *refs: pack_kernel(rows, *refs),
        name="packed",
        out_shape=jax.ShapeDtypeStruct((length, height, width), BF16),
        in_specs=in_vmem(5),
        out_specs=pl.BlockSpec(memory_space=pltpu.VMEM),
        compiler_params=pltpu.CompilerParams(vmem_limit_bytes=12 * MIB),
    )(*pieces)


def merged(arrived_ref, at, wide):
    lines = arrived_ref[...].astype(F32)
    parts = sum(lines[:, at + j * wide : at + (j + 1) * wide] for j in range(3))
    top = jnp.max(parts, axis=0)
    logs = top + jnp.log(jnp.sum(jnp.exp(parts - top[None]), axis=0))
    return lines, jnp.exp(parts - logs[None]), logs


def middle_kernel(rows, plane_ref, arrived_ref, out_ref, turned, built):
    length = arrived_ref.shape[0]
    depth, height, width = out_ref.shape
    chips = length * depth
    wide = 2 * rows * chips // width
    kept = rows * depth
    lines, scale, logs = merged(arrived_ref, 2 * kept, wide)
    scale = scale.reshape(length * wide, width)
    pad = jnp.zeros((-(length * wide) % 128, width), F32)
    turned[...] = jnp.concatenate([scale, pad]).T
    for k in range(rows):
        c, lane = k * chips // width, k * chips % width
        across = turned[pl.ds(pl.multiple_of(plane_ref[0] * depth + lane, depth), depth), :]
        grad = jnp.zeros((depth, width), F32)
        picked = jnp.zeros((depth, width), F32)
        for j in range(length):
            at = j * wide + c
            grad += lines[j, k * depth : (k + 1) * depth] * across[:, at : at + 1]
            picked += lines[j, kept + k * depth : kept + (k + 1) * depth]
        for z in range(depth):
            built[z, k : k + 1, :] = grad[z : z + 1]
            built[z, rows + k : rows + k + 1, :] = picked[z : z + 1]
    lines = jnp.concatenate(three_parts(logs))
    at = 2 * rows
    built[:, at : at + 3 * wide, :] = jnp.broadcast_to(lines[None], (depth, 3 * wide, width))
    at += 3 * wide
    if height > at:
        built[:, at:, :] = jnp.zeros((depth, height - at, width), F32)
    out_ref[...] = built[...].astype(BF16)


def middle(rows, depth, plane, arrived):
    length, _, width = arrived.shape
    wide = 2 * rows * length * depth // width
    height = 2 * rows + 3 * wide
    height += -height % 8
    return pl.pallas_call(
        lambda *refs: middle_kernel(rows, *refs),
        name="middle",
        out_shape=jax.ShapeDtypeStruct((depth, height, width), BF16),
        in_specs=[pl.BlockSpec(memory_space=pltpu.SMEM), *in_vmem(1)],
        out_specs=pl.BlockSpec(memory_space=pltpu.VMEM),
        scratch_shapes=[
            pltpu.VMEM((width, length * wide + -(length * wide) % 128), F32),
            pltpu.VMEM((depth, height, width), F32),
        ],
        compiler_params=pltpu.CompilerParams(vmem_limit_bytes=12 * MIB),
    )(plane, arrived)


def last_kernel(
    chip_ref, arrived_ref, place_ref, far_place_ref, weight_ref, hidden_ref, states_ref,
    far_states_ref, items_ref, loss_hbm, hidden_grad_hbm, table_grad_hbm,
    states, buffer, loss_ref, hidden_grad_ref, sems,
):
    rows, width = hidden_ref.shape
    depth = arrived_ref.shape[0]
    items = items_ref.shape[0]
    count = states.shape[0]
    block = min(BLOCK, items)
    chips = count // (2 * rows)
    wide = count // width
    copies = []

    def send(source, target):
        copies.append(pltpu.make_async_copy(source, target, sems.at[len(copies)]))
        copies[-1].start()

    lines, scale, logs = merged(arrived_ref, 2 * rows, wide)
    weight = weight_ref[...]
    lane = lax.broadcasted_iota(jnp.int32, (1, width), 1)
    hidden = hidden_ref[...].astype(F32)
    place = lax.broadcasted_iota(jnp.int32, loss_ref.shape, 1)
    losses = jnp.zeros(loss_ref.shape, F32)
    grads = []
    for k in range(rows):
        c, first = k * chips // width, k * chips % width
        mine = lambda x: jnp.sum(
            jnp.where(lane == chip_ref[0] + first, x, 0.0), axis=-1, keepdims=True
        )
        log_total = mine(logs[c : c + 1])
        own_weight = mine(weight[:, c * width : (c + 1) * width])
        grad = jnp.zeros((1, width), F32)
        picked = jnp.zeros((1, width), F32)
        for j in range(depth):
            grad += lines[j, k : k + 1] * mine(scale[j, c : c + 1])
            picked += lines[j, rows + k : rows + k + 1]
        score = jnp.sum(hidden[k : k + 1] * picked, axis=1, keepdims=True)
        losses = jnp.where(place == k, log_total - score, losses)
        pull = (own_weight * (jnp.exp(score - log_total) - 1.0)).astype(BF16).astype(F32)
        grads.append(own_weight * grad + pull * picked)
    loss_ref[...] = losses
    send(loss_ref, loss_hbm)
    hidden_grad_ref[...] = jnp.concatenate(grads).astype(BF16)
    send(hidden_grad_ref, hidden_grad_hbm)
    line = jnp.concatenate([logs[c : c + 1] for c in range(wide)], axis=1)
    places = jnp.concatenate([place_ref[...], far_place_ref[...]], axis=1)
    states[: count // 2, :] = states_ref[...]
    states[count // 2 :, :] = far_states_ref[...]
    for at in range(0, items, block):
        scores = lax.dot_general(
            items_ref[at : at + block, :], states[...], (((1,), (1,)), ((), ())),
            preferred_element_type=F32,
        )
        parts = jnp.exp(scores - line)
        matched = lax.broadcasted_iota(jnp.int32, parts.shape, 0) == places - at
        signal = (weight * jnp.where(matched, parts - 1.0, parts)).astype(BF16)
        buffer[at : at + block, :] = jnp.dot(
            signal, states[...], preferred_element_type=F32
        ).astype(BF16)
        send(buffer.at[pl.ds(at, block)], table_grad_hbm.at[pl.ds(at, block)])
    for copy in copies:
        copy.wait()


def last(chip, arrived, place, far_place, weight, hidden, states, far_states, items):
    rows, width = hidden.shape
    return pl.pallas_call(
        last_kernel,
        name="last",
        out_shape=(
            jax.ShapeDtypeStruct((1, rows), F32),
            jax.ShapeDtypeStruct((rows, width), BF16),
            jax.ShapeDtypeStruct(items.shape, BF16),
        ),
        in_specs=[pl.BlockSpec(memory_space=pltpu.SMEM), *in_vmem(8)],
        out_specs=[pl.BlockSpec(memory_space=pltpu.HBM)] * 3,
        scratch_shapes=[
            pltpu.VMEM((2 * states.shape[0], width), BF16),
            pltpu.VMEM(items.shape, BF16),
            pltpu.VMEM((1, rows), F32),
            pltpu.VMEM((rows, width), BF16),
            pltpu.SemaphoreType.DMA((2 + items.shape[0] // min(BLOCK, items.shape[0]),)),
        ],
        compiler_params=pltpu.CompilerParams(vmem_limit_bytes=16 * MIB),
    )(chip, arrived, place, far_place, weight, hidden, states, far_states, items)


def steps(hidden, item_table, targets, lengths):
    rows, _ = hidden.shape
    group = lax.axis_index("grp")
    chip = lax.axis_index(CHIPS).reshape(1)
    own_items = item_table.shape[0] // 2
    items = lax.dynamic_slice_in_dim(item_table, group * own_items, own_items)
    first_own = (lax.axis_index(ITEM) * 2 + group) * own_items
    weight = weights_for(lengths, rows)
    sent = spread(hidden, targets, lax.axis_size(CHIPS))
    mine = lax.all_to_all(sent, CHIPS, 0, 0, tiled=True)
    mine = jnp.swapaxes(mine, 0, 1)
    first_own = first_own.reshape(1)
    other = from_pair(mine)
    no_logs = jnp.zeros((1, rows * lax.axis_size(CHIPS)), F32)
    own_logs, place, states, own_grad, own_picked = shares(False, first_own, mine, items, no_logs)
    far_logs, far_place, far_states, far_share = shares(
        True, first_own, other, items, own_logs
    )
    sent = packed(
        rows, lax.axis_size(PLANE), own_grad, own_picked, from_pair(far_share),
        own_logs, far_logs,
    )
    arrived = lax.all_to_all(sent, PLANE, 0, 0, tiled=True)
    sent = middle(rows, lax.axis_size("z"), lax.axis_index(PLANE).reshape(1), arrived)
    arrived = lax.all_to_all(sent, "z", 0, 0, tiled=True)
    row_loss, hidden_grad, table_grad = last(
        chip, arrived, place, far_place, weight, hidden, states, far_states, items
    )
    return (row_loss.reshape(-1), hidden_grad, table_grad)


def mapped(split):
    return jax.shard_map(
        steps,
        mesh=split,
        in_specs=(P(GRP_ITEM, None), P(ITEM, None), P(GRP_ITEM), P()),
        out_specs=(P(GRP_ITEM), P(GRP_ITEM, None), P(ITEM_GRP, None)),
        check_vma=False,
    )


def solution(mesh):
    split = Mesh(
        mesh.devices.reshape(4, 2, 8, 2, mesh.shape["grp"]),
        ("x", "yh", "z", "core", "grp"),
    )
    return mapped(split)
```

```python
import jax
import jax.numpy as jnp
from jax import lax
from jax.experimental import pallas as pl
from jax.experimental.pallas import tpu as pltpu
from jax.sharding import Mesh
from jax.sharding import PartitionSpec as P

ITEM = ("x", "yh", "z", "core")
GRP_ITEM = ("grp", "x", "yh", "z", "core")
ITEM_GRP = ("x", "yh", "z", "core", "grp")
PLANE = ("x", "yh", "grp")
CHIPS = ("x", "yh", "grp", "z")
DIGIT = 128
BLOCK = 512
MIB = 1 << 20
F32 = jnp.float32
BF16 = jnp.bfloat16


def from_pair(x):
    return lax.ppermute(x, "core", [(0, 1), (1, 0)])


def spread_kernel(targets_hbm, hidden_hbm, out_ref, targets_ref, hidden_ref, sems):
    copies = [
        pltpu.make_async_copy(targets_hbm, targets_ref, sems.at[0]),
        pltpu.make_async_copy(hidden_hbm, hidden_ref, sems.at[1]),
    ]
    for copy in copies:
        copy.start()
    for copy in copies:
        copy.wait()
    _, height, width = out_ref.shape
    rows = height - 1
    lane = lax.broadcasted_iota(jnp.int32, (1, width), 1)
    digits = jnp.zeros((1, width), jnp.int32)
    for k in range(rows):
        rest = targets_ref[k]
        for j in range(3):
            digits = jnp.where(lane == j * rows + k, rest % DIGIT, digits)
            rest = rest // DIGIT
    line = jnp.concatenate([hidden_ref[...].astype(F32), digits.astype(F32)])
    out_ref[...] = jnp.broadcast_to(line[None], out_ref.shape).astype(BF16)


def spread(hidden, targets, chips):
    rows, width = hidden.shape
    return pl.pallas_call(
        spread_kernel,
        name="spread",
        out_shape=jax.ShapeDtypeStruct((chips, rows + 1, width), BF16),
        in_specs=[pl.BlockSpec(memory_space=pltpu.HBM)] * 2,
        out_specs=pl.BlockSpec(memory_space=pltpu.VMEM),
        scratch_shapes=[
            pltpu.SMEM(targets.shape, jnp.int32),
            pltpu.VMEM(hidden.shape, BF16),
            pltpu.SemaphoreType.DMA((2,)),
        ],
        compiler_params=pltpu.CompilerParams(vmem_limit_bytes=4 * MIB),
    )(in_hbm(targets), in_hbm(hidden))


def in_hbm(x):
    return pltpu.with_memory_space_constraint(x, pltpu.HBM)


def in_vmem(count):
    return [pl.BlockSpec(memory_space=pltpu.VMEM) for _ in range(count)]


def weights_for(lengths, rows):
    groups, seq_count = lengths.shape
    cores, x, yh, grps, z = (lax.axis_size(axis) for axis in ("core", "x", "yh", "grp", "z"))
    half, k, at_x, at_yh, at_grp, at_z = jnp.unravel_index(
        jnp.arange(cores * rows * x * yh * grps * z), (cores, rows, x, yh, grps, z)
    )
    core = (half + lax.axis_index("core")) % cores
    place = (((at_x * yh + at_yh) * z + at_z) * cores + core) * rows + k
    group_rows = place.shape[0] // groups
    before = jnp.arange(seq_count)[:, None] < jnp.arange(seq_count)[None, :]
    starts = jnp.sum(jnp.where(before[None], lengths[:, :, None], 0), axis=1)
    inside = (
        (at_grp[:, None, None] == jnp.arange(groups)[None, :, None])
        & (place[:, None, None] >= starts[None])
        & (place[:, None, None] < (starts + lengths)[None])
    )
    row_length = jnp.sum(jnp.where(inside, lengths[None].astype(F32), F32(0.0)), axis=(1, 2))
    return (group_rows / seq_count / row_length).reshape(1, -1)


def column(line):
    return jnp.broadcast_to(line, (128, line.shape[1])).T[:, :1]


def three_parts(x):
    high = x.astype(BF16).astype(F32)
    rest = x - high
    middle = rest.astype(BF16).astype(F32)
    return [high, middle, rest - middle]


def share_kernel(
    far, first_ref, given_ref, items_ref, near_log_ref, log_ref, place_ref, states_ref, grad_ref,
    *rest,
):
    scores, places, grad, picked = rest[-4:]
    rows = given_ref.shape[0] - 1
    chips = given_ref.shape[1]
    count, width = states_ref.shape
    items = items_ref.shape[0]
    block = min(BLOCK, items)
    lanes = min(128, block)
    digits = given_ref[rows].astype(F32)
    across = digits.T
    for k in range(rows):
        at = k * chips
        states_ref[at : at + chips, :] = given_ref[k]
        found = [digits[:, j * rows + k : j * rows + k + 1].astype(jnp.int32) for j in range(3)]
        found = found[0] + DIGIT * found[1] + DIGIT**2 * found[2] - first_ref[0]
        places[at : at + chips, :] = jnp.broadcast_to(found, (chips, lanes))
        found = [across[j * rows + k : j * rows + k + 1, :].astype(jnp.int32) for j in range(3)]
        found = found[0] + DIGIT * found[1] + DIGIT**2 * found[2] - first_ref[0]
        place_ref[:, at : at + chips] = found
    states = states_ref[...]
    high = None
    for at in range(0, items, block):
        found = lax.dot_general(
            states, items_ref[at : at + block, :], (((1,), (1,)), ((), ())), preferred_element_type=F32
        )
        scores[:, at : at + block] = found
        for c in range(0, block, lanes):
            top = found[:, c : c + lanes]
            high = top if high is None else jnp.maximum(high, top)
    high = jnp.max(high, axis=1, keepdims=True)
    total = None
    lane = lax.broadcasted_iota(jnp.int32, (1, lanes), 1)
    for at in range(0, items, block):
        others, hot = [], []
        for c in range(at, at + block, lanes):
            parts = jnp.exp(scores[:, c : c + lanes] - high)
            total = parts if total is None else total + parts
            matched = places[...] == lane + c
            others.append(jnp.where(matched, 0.0, parts).astype(BF16))
            hot.append(jnp.where(matched, 1.0, 0.0).astype(BF16))
        table = items_ref[at : at + block, :]
        more = jnp.dot(jnp.concatenate(others, axis=1), table, preferred_element_type=F32)
        grad[...] = more if at == 0 else grad[...] + more
        more = jnp.dot(jnp.concatenate(hot, axis=1), table, preferred_element_type=F32)
        picked[...] = more if at == 0 else picked[...] + more
    log_sum = high + jnp.log(jnp.sum(total, axis=1, keepdims=True))
    line = jnp.broadcast_to(log_sum, (count, 128)).T[:1, :]
    log_ref[...] = line
    share = grad[...] * jnp.exp(high - log_sum)
    if not far:
        grad_ref[...] = share
        rest[0][...] = picked[...].astype(BF16)
        return
    grad_ref[:count, :] = share.astype(BF16)
    grad_ref[count : 2 * count, :] = picked[...].astype(BF16)
    lines = [
        piece[:, at : at + chips]
        for source in (line, near_log_ref[...])
        for piece in three_parts(source)
        for at in range(0, count, chips)
    ]
    lines = jnp.concatenate(lines + [jnp.zeros((-len(lines) % 16, chips), F32)])
    lines = jnp.concatenate([lines, jnp.zeros((lines.shape[0], width - chips), F32)], axis=1)
    grad_ref[2 * count :, :] = lines.astype(BF16)


def shares(far, first, given, items, near_logs):
    height, chips, width = given.shape
    count = (height - 1) * chips
    lines = 6 * (height - 1)
    results = [
        jax.ShapeDtypeStruct((1, count), F32),
        jax.ShapeDtypeStruct((1, count), jnp.int32),
        jax.ShapeDtypeStruct((count, width), BF16),
    ]
    if far:
        results += [jax.ShapeDtypeStruct((2 * count + lines + -lines % 16, width), BF16)]
    else:
        results += [
            jax.ShapeDtypeStruct((count, width), F32),
            jax.ShapeDtypeStruct((count, width), BF16),
        ]
    return pl.pallas_call(
        lambda *refs: share_kernel(far, *refs),
        name="shares",
        out_shape=results,
        in_specs=[pl.BlockSpec(memory_space=pltpu.SMEM), *in_vmem(3)],
        out_specs=in_vmem(len(results)),
        scratch_shapes=[
            pltpu.VMEM((count, items.shape[0]), F32),
            pltpu.VMEM((count, min(128, BLOCK)), jnp.int32),
            pltpu.VMEM((count, width), F32),
            pltpu.VMEM((count, width), F32),
        ],
        compiler_params=pltpu.CompilerParams(vmem_limit_bytes=24 * MIB),
    )(first, given, items, near_logs)


def pack_kernel(
    rows, own_grad_ref, own_rows_ref, other_ref, own_log_ref, far_log_ref, out_ref
):
    length, _, width = out_ref.shape
    part = own_grad_ref.shape[0]
    own = jnp.concatenate([own_log_ref[...], far_log_ref[...]], axis=1)
    lines = other_ref[2 * part :, :].astype(F32)
    chips = part // rows
    other = [
        sum(lines[at + j * rows + k : at + j * rows + k + 1, :chips] for j in range(3))
        for at in (0, 3 * rows)
        for k in range(rows)
    ]
    other = jnp.concatenate(other, axis=1)
    top = jnp.maximum(own, other)
    both = top + jnp.log(jnp.exp(own - top) + jnp.exp(other - top))
    grad = own_grad_ref[...] * column(jnp.exp(own - both)[:, :part])
    grad += other_ref[:part, :].astype(F32) * column(jnp.exp(other - both)[:, :part])
    picked = own_rows_ref[...].astype(F32) + other_ref[part : 2 * part, :].astype(F32)
    lines = [
        piece[:, at : at + width] for piece in three_parts(both) for at in range(0, 2 * part, width)
    ]
    lines = jnp.concatenate(lines)
    across = lambda x: [
        x.reshape(rows, length, -1, width)[k] for k in range(rows)
    ]
    sent = across(grad) + across(picked) + [jnp.broadcast_to(lines[None], (length, *lines.shape))]
    out_ref[...] = jnp.concatenate(sent, axis=1).astype(BF16)


def packed(rows, length, *pieces):
    part, width = pieces[0].shape
    lines = 3 * 2 * part // width
    height = 2 * (part // length) + lines
    return pl.pallas_call(
        lambda *refs: pack_kernel(rows, *refs),
        name="packed",
        out_shape=jax.ShapeDtypeStruct((length, height, width), BF16),
        in_specs=in_vmem(5),
        out_specs=pl.BlockSpec(memory_space=pltpu.VMEM),
        compiler_params=pltpu.CompilerParams(vmem_limit_bytes=12 * MIB),
    )(*pieces)


def merged(arrived_ref, at, wide):
    lines = arrived_ref[...].astype(F32)
    parts = sum(lines[:, at + j * wide : at + (j + 1) * wide] for j in range(3))
    top = jnp.max(parts, axis=0)
    logs = top + jnp.log(jnp.sum(jnp.exp(parts - top[None]), axis=0))
    return lines, jnp.exp(parts - logs[None]), logs


def middle_kernel(rows, plane_ref, arrived_ref, out_ref, turned, built):
    length = arrived_ref.shape[0]
    depth, height, width = out_ref.shape
    chips = length * depth
    wide = 2 * rows * chips // width
    kept = rows * depth
    lines, scale, logs = merged(arrived_ref, 2 * kept, wide)
    scale = scale.reshape(length * wide, width)
    pad = jnp.zeros((-(length * wide) % 128, width), F32)
    turned[...] = jnp.concatenate([scale, pad]).T
    for k in range(rows):
        c, lane = k * chips // width, k * chips % width
        across = turned[pl.ds(pl.multiple_of(plane_ref[0] * depth + lane, depth), depth), :]
        grad = jnp.zeros((depth, width), F32)
        picked = jnp.zeros((depth, width), F32)
        for j in range(length):
            at = j * wide + c
            grad += lines[j, k * depth : (k + 1) * depth] * across[:, at : at + 1]
            picked += lines[j, kept + k * depth : kept + (k + 1) * depth]
        for z in range(depth):
            built[z, k : k + 1, :] = grad[z : z + 1]
            built[z, rows + k : rows + k + 1, :] = picked[z : z + 1]
    lines = jnp.concatenate(three_parts(logs))
    at = 2 * rows
    built[:, at : at + 3 * wide, :] = jnp.broadcast_to(lines[None], (depth, 3 * wide, width))
    at += 3 * wide
    if height > at:
        built[:, at:, :] = jnp.zeros((depth, height - at, width), F32)
    out_ref[...] = built[...].astype(BF16)


def middle(rows, depth, plane, arrived):
    length, _, width = arrived.shape
    wide = 2 * rows * length * depth // width
    height = 2 * rows + 3 * wide
    height += -height % 8
    return pl.pallas_call(
        lambda *refs: middle_kernel(rows, *refs),
        name="middle",
        out_shape=jax.ShapeDtypeStruct((depth, height, width), BF16),
        in_specs=[pl.BlockSpec(memory_space=pltpu.SMEM), *in_vmem(1)],
        out_specs=pl.BlockSpec(memory_space=pltpu.VMEM),
        scratch_shapes=[
            pltpu.VMEM((width, length * wide + -(length * wide) % 128), F32),
            pltpu.VMEM((depth, height, width), F32),
        ],
        compiler_params=pltpu.CompilerParams(vmem_limit_bytes=12 * MIB),
    )(plane, arrived)


def last_kernel(
    chip_ref, arrived_ref, place_ref, far_place_ref, weight_ref, hidden_ref, states_ref,
    far_states_ref, items_ref, loss_hbm, hidden_grad_hbm, table_grad_hbm,
    states, buffer, loss_ref, hidden_grad_ref, sems,
):
    rows, width = hidden_ref.shape
    depth = arrived_ref.shape[0]
    items = items_ref.shape[0]
    count = states.shape[0]
    block = min(BLOCK, items)
    chips = count // (2 * rows)
    wide = count // width
    copies = []

    def send(source, target):
        copies.append(pltpu.make_async_copy(source, target, sems.at[len(copies)]))
        copies[-1].start()

    lines, scale, logs = merged(arrived_ref, 2 * rows, wide)
    weight = weight_ref[...]
    lane = lax.broadcasted_iota(jnp.int32, (1, width), 1)
    hidden = hidden_ref[...].astype(F32)
    place = lax.broadcasted_iota(jnp.int32, loss_ref.shape, 1)
    losses = jnp.zeros(loss_ref.shape, F32)
    grads = []
    for k in range(rows):
        c, first = k * chips // width, k * chips % width
        mine = lambda x: jnp.sum(
            jnp.where(lane == chip_ref[0] + first, x, 0.0), axis=-1, keepdims=True
        )
        log_total = mine(logs[c : c + 1])
        own_weight = mine(weight[:, c * width : (c + 1) * width])
        grad = jnp.zeros((1, width), F32)
        picked = jnp.zeros((1, width), F32)
        for j in range(depth):
            grad += lines[j, k : k + 1] * mine(scale[j, c : c + 1])
            picked += lines[j, rows + k : rows + k + 1]
        score = jnp.sum(hidden[k : k + 1] * picked, axis=1, keepdims=True)
        losses = jnp.where(place == k, log_total - score, losses)
        pull = (own_weight * (jnp.exp(score - log_total) - 1.0)).astype(BF16).astype(F32)
        grads.append(own_weight * grad + pull * picked)
    loss_ref[...] = losses
    send(loss_ref, loss_hbm)
    hidden_grad_ref[...] = jnp.concatenate(grads).astype(BF16)
    send(hidden_grad_ref, hidden_grad_hbm)
    line = jnp.concatenate([logs[c : c + 1] for c in range(wide)], axis=1)
    weighted = line - jnp.log(weight)
    places = jnp.concatenate([place_ref[...], far_place_ref[...]], axis=1)
    states[: count // 2, :] = states_ref[...]
    states[count // 2 :, :] = far_states_ref[...]
    for at in range(0, items, block):
        scores = lax.dot_general(
            items_ref[at : at + block, :], states[...], (((1,), (1,)), ((), ())),
            preferred_element_type=F32,
        )
        parts = jnp.exp(scores - weighted)
        matched = lax.broadcasted_iota(jnp.int32, parts.shape, 0) == places - at
        signal = jnp.where(matched, parts - weight, parts).astype(BF16)
        buffer[at : at + block, :] = jnp.dot(
            signal, states[...], preferred_element_type=F32
        ).astype(BF16)
        send(buffer.at[pl.ds(at, block)], table_grad_hbm.at[pl.ds(at, block)])
    for copy in copies:
        copy.wait()


def last(chip, arrived, place, far_place, weight, hidden, states, far_states, items):
    rows, width = hidden.shape
    return pl.pallas_call(
        last_kernel,
        name="last",
        out_shape=(
            jax.ShapeDtypeStruct((1, rows), F32),
            jax.ShapeDtypeStruct((rows, width), BF16),
            jax.ShapeDtypeStruct(items.shape, BF16),
        ),
        in_specs=[pl.BlockSpec(memory_space=pltpu.SMEM), *in_vmem(8)],
        out_specs=[pl.BlockSpec(memory_space=pltpu.HBM)] * 3,
        scratch_shapes=[
            pltpu.VMEM((2 * states.shape[0], width), BF16),
            pltpu.VMEM(items.shape, BF16),
            pltpu.VMEM((1, rows), F32),
            pltpu.VMEM((rows, width), BF16),
            pltpu.SemaphoreType.DMA((2 + items.shape[0] // min(BLOCK, items.shape[0]),)),
        ],
        compiler_params=pltpu.CompilerParams(vmem_limit_bytes=16 * MIB),
    )(chip, arrived, place, far_place, weight, hidden, states, far_states, items)


def steps(hidden, item_table, targets, lengths):
    rows, _ = hidden.shape
    group = lax.axis_index("grp")
    chip = lax.axis_index(CHIPS).reshape(1)
    own_items = item_table.shape[0] // 2
    items = lax.dynamic_slice_in_dim(item_table, group * own_items, own_items)
    first_own = (lax.axis_index(ITEM) * 2 + group) * own_items
    weight = weights_for(lengths, rows)
    sent = spread(hidden, targets, lax.axis_size(CHIPS))
    mine = lax.all_to_all(sent, CHIPS, 0, 0, tiled=True)
    mine = jnp.swapaxes(mine, 0, 1)
    first_own = first_own.reshape(1)
    other = from_pair(mine)
    no_logs = jnp.zeros((1, rows * lax.axis_size(CHIPS)), F32)
    own_logs, place, states, own_grad, own_picked = shares(False, first_own, mine, items, no_logs)
    far_logs, far_place, far_states, far_share = shares(
        True, first_own, other, items, own_logs
    )
    sent = packed(
        rows, lax.axis_size(PLANE), own_grad, own_picked, from_pair(far_share),
        own_logs, far_logs,
    )
    arrived = lax.all_to_all(sent, PLANE, 0, 0, tiled=True)
    sent = middle(rows, lax.axis_size("z"), lax.axis_index(PLANE).reshape(1), arrived)
    arrived = lax.all_to_all(sent, "z", 0, 0, tiled=True)
    row_loss, hidden_grad, table_grad = last(
        chip, arrived, place, far_place, weight, hidden, states, far_states, items
    )
    return (row_loss.reshape(-1), hidden_grad, table_grad)


def mapped(split):
    return jax.shard_map(
        steps,
        mesh=split,
        in_specs=(P(GRP_ITEM, None), P(ITEM, None), P(GRP_ITEM), P()),
        out_specs=(P(GRP_ITEM), P(GRP_ITEM, None), P(ITEM_GRP, None)),
        check_vma=False,
    )


def solution(mesh):
    split = Mesh(
        mesh.devices.reshape(4, 2, 8, 2, mesh.shape["grp"]),
        ("x", "yh", "z", "core", "grp"),
    )
    return mapped(split)
```
